32 devices in a mesh: dp: 8 (over y, x, core), branch: 4 (over z).
Axes of the slice: x: 2, y: 2, z: 4, core: 2. Of those that a mesh axis runs over, the one named last changes fastest.
Arguments:
- image_hidden: bfloat16 [4096, 1024], P('dp', 'branch'), may hold values from -8 to 8
- text_hidden: bfloat16 [4096, 768], P('dp', 'branch'), may hold values from -8 to 8
- image_proj: bfloat16 [1024, 768], replicated, may hold values from -0.1875 to 0.1875
- text_proj: bfloat16 [768, 768], replicated, may hold values from -0.21650635 to 0.21650635
- log_inverse_sharpness: float32 [1], replicated, may hold values from 4 to 5.9
- partner: int32 [4096], replicated, may hold values from 0 to 4095, each once
Outputs:
- loss: float32 [1], replicated
- grad_log_scale: float32 [1], replicated
- grad_image_hidden: bfloat16 [4096, 1024], P('dp', 'branch')
- grad_text_hidden: bfloat16 [4096, 768], P('dp', 'branch')
- grad_image_proj: float32 [1024, 768], P('branch')
- grad_text_proj: float32 [768, 768], P('branch')
The draws below stay inside these ranges and needn't reach their ends.
Inputs may be any that keep to these rules, and one draw needn't show every extreme that they name: `partner`: each text index appears exactly once.
All inputs are finite; a program needn't handle non-finite values.
Results may differ from the reference program's by a relative error of at most 0.0029.
The reference program's roundings to bfloat16 on the way count: a program that leaves them out, or rounds other values in their place, can miss the bound.
Values may be sent and summed in bfloat16 or wider, within the bound.
A program may use at most 64 MiB of HBM per device.

```python
import jax
import jax.numpy as jnp
from jax import lax

IMG_WIDTH = 1024
TXT_WIDTH = 768
EMBED = 768
PAIRS = 4096
N_DP = 8


def joint_draw(key):
    streams = jax.random.split(jax.random.fold_in(key, 7), 4)
    image_proj = jax.random.truncated_normal(streams[0], -6.0, 6.0, (IMG_WIDTH, EMBED), jnp.float32) * IMG_WIDTH ** (-0.5)
    text_proj = jax.random.truncated_normal(streams[1], -6.0, 6.0, (TXT_WIDTH, EMBED), jnp.float32) * TXT_WIDTH ** (-0.5)
    image_hidden = jax.random.truncated_normal(streams[2], -6.0, 6.0, (PAIRS, IMG_WIDTH), jnp.float32)
    text_hidden = jax.random.truncated_normal(streams[3], -6.0, 6.0, (PAIRS, TXT_WIDTH), jnp.float32)
    image_hidden = jnp.clip(image_hidden, -8.0, 8.0)
    text_hidden = jnp.clip(text_hidden, -8.0, 8.0)
    return (image_hidden, text_hidden, image_proj, text_proj)


def draw_image_hidden(key, part):
    return joint_draw(key)[0].astype(jnp.bfloat16)


def draw_text_hidden(key, part):
    return joint_draw(key)[1].astype(jnp.bfloat16)


def draw_image_proj(key, part):
    return joint_draw(key)[2].astype(jnp.bfloat16)


def draw_text_proj(key, part):
    return joint_draw(key)[3].astype(jnp.bfloat16)


def draw_log_inverse_sharpness(key, part):
    stream = jax.random.fold_in(key, 11)
    return jax.random.uniform(stream, (1,), jnp.float32, 4.0, 5.9)


def setup_inputs(seed: int = 0) -> dict:
    keys = jax.random.split(jax.random.key(seed), 7)
    image_hidden = draw_image_hidden(jax.random.fold_in(keys[6], 71), 0)
    text_hidden = draw_text_hidden(jax.random.fold_in(keys[6], 71), 0)
    image_proj = draw_image_proj(jax.random.fold_in(keys[6], 71), 0)
    text_proj = draw_text_proj(jax.random.fold_in(keys[6], 71), 0)
    log_inverse_sharpness = draw_log_inverse_sharpness(jax.random.fold_in(keys[6], 71), 0)
    partner = jax.random.permutation(keys[5], PAIRS).astype(jnp.int32)
    return dict(image_hidden=image_hidden, text_hidden=text_hidden, image_proj=image_proj, text_proj=text_proj, log_inverse_sharpness=log_inverse_sharpness, partner=partner)


NORM_EPSILON = 1e-06

def normalize(raw_rows):
    lengths = jnp.sqrt(lax.optimization_barrier(jnp.sum(raw_rows * raw_rows, axis=1, keepdims=True)) + NORM_EPSILON)
    unit_rows = raw_rows / lengths
    return (unit_rows, lengths, unit_rows.astype(jnp.bfloat16))

def unnormalize(upstream, unit_rows, lengths):
    radial = lax.optimization_barrier(jnp.sum(upstream * unit_rows, axis=1, keepdims=True))
    return ((upstream - unit_rows * radial) / lengths).astype(jnp.bfloat16)

def reference(image_hidden, text_hidden, image_proj, text_proj, log_inverse_sharpness, partner):
    total_pairs = image_hidden.shape[0]
    image_raw = jnp.dot(image_hidden.astype(jnp.float32), image_proj.astype(jnp.float32), preferred_element_type=jnp.float32)
    text_raw = jnp.dot(text_hidden.astype(jnp.float32), text_proj.astype(jnp.float32), preferred_element_type=jnp.float32)
    image_unit, image_length, image_emb = normalize(image_raw)
    text_unit, text_length, caption_feature_entries = normalize(text_raw)
    normalized_exponent_divisor = jnp.exp(log_inverse_sharpness[0])
    block_rows = total_pairs // N_DP
    image_blocks = image_emb.reshape(N_DP, block_rows, -1)
    partner_blocks = partner.reshape(N_DP, block_rows)
    column_ids = jnp.arange(total_pairs, dtype=jnp.int32)
    denominator = 2.0 * total_pairs

    def block_logits(sample_feature_entries):
        return normalized_exponent_divisor * lax.dot_general(sample_feature_entries.astype(jnp.float32), caption_feature_entries.astype(jnp.float32), (((1,), (1,)), ((), ())), preferred_element_type=jnp.float32)

    def forward(carried, item):
        column_peak, column_mass = carried
        sample_feature_entries, rows_partner = item
        matching_cosine_scores = block_logits(sample_feature_entries)
        row_peak = lax.optimization_barrier(jnp.max(matching_cosine_scores, axis=1))
        row_lse = row_peak + jnp.log(lax.optimization_barrier(jnp.sum(jnp.exp(matching_cosine_scores - row_peak[:, None]), axis=1)))
        matched = rows_partner[:, None] == column_ids[None, :]
        positive = lax.optimization_barrier(jnp.sum(jnp.where(matched, matching_cosine_scores, 0.0), axis=1))
        new_peak = jnp.maximum(column_peak, lax.optimization_barrier(jnp.max(matching_cosine_scores, axis=0)))
        column_mass = column_mass * jnp.exp(column_peak - new_peak) + lax.optimization_barrier(jnp.sum(jnp.exp(matching_cosine_scores - new_peak[None, :]), axis=0))
        return ((new_peak, column_mass), (row_lse, positive))
    start_peak = jnp.full((total_pairs,), -jnp.inf, jnp.float32)
    start_mass = jnp.zeros((total_pairs,), jnp.float32)
    (column_peak, column_mass), (row_lse, positive) = lax.scan(forward, (start_peak, start_mass), (image_blocks, partner_blocks))
    col_lse = column_peak + jnp.log(column_mass)
    loss = (jnp.sum(row_lse) + jnp.sum(col_lse) - 2.0 * jnp.sum(positive)) / denominator

    def backward(carried, item):
        caption_objective_sum, scale_total = carried
        sample_feature_entries, rows_partner, rows_lse = item
        matching_cosine_scores = block_logits(sample_feature_entries)
        matched = (rows_partner[:, None] == column_ids[None, :]).astype(jnp.float32)
        weights = (jnp.exp(matching_cosine_scores - rows_lse[:, None]) + jnp.exp(matching_cosine_scores - col_lse[None, :]) - 2.0 * matched) / denominator
        scale_total = scale_total + jnp.sum(weights * matching_cosine_scores)
        reduced_width_parameters = weights.astype(jnp.bfloat16)
        picture_projection_matrix = normalized_exponent_divisor * jnp.dot(reduced_width_parameters.astype(jnp.float32), caption_feature_entries.astype(jnp.float32), preferred_element_type=jnp.float32)
        caption_objective_sum = caption_objective_sum + normalized_exponent_divisor * lax.dot_general(reduced_width_parameters.astype(jnp.float32), sample_feature_entries.astype(jnp.float32), (((0,), (0,)), ((), ())), preferred_element_type=jnp.float32)
        return ((caption_objective_sum, scale_total), picture_projection_matrix)
    start_text = jnp.zeros((total_pairs, caption_feature_entries.shape[1]), jnp.float32)
    start_scale = jnp.zeros((), jnp.float32)
    (text_up, scale_grad), picture_projection_matrix = lax.scan(backward, (start_text, start_scale), (image_blocks, partner_blocks, row_lse))
    picture_projection_matrix = picture_projection_matrix.reshape(total_pairs, -1)
    image_down = unnormalize(picture_projection_matrix, image_unit, image_length)
    text_down = unnormalize(text_up, text_unit, text_length)
    grad_image_hidden = jnp.dot(image_down.astype(jnp.float32), image_proj.T.astype(jnp.float32), preferred_element_type=jnp.float32).astype(jnp.bfloat16)
    grad_text_hidden = jnp.dot(text_down.astype(jnp.float32), text_proj.T.astype(jnp.float32), preferred_element_type=jnp.float32).astype(jnp.bfloat16)
    grad_image_proj = jnp.dot(image_hidden.T.astype(jnp.float32), image_down.astype(jnp.float32), preferred_element_type=jnp.float32)
    grad_text_proj = jnp.dot(text_hidden.T.astype(jnp.float32), text_down.astype(jnp.float32), preferred_element_type=jnp.float32)
    return (loss.reshape(1), scale_grad.reshape(1), grad_image_hidden, grad_text_hidden, grad_image_proj, grad_text_proj)
```

```python
import functools

import jax
import jax.numpy as jnp
from jax import lax
from jax.experimental import pallas as pl
from jax.experimental.pallas import tpu as pltpu
from jax.sharding import PartitionSpec as P

NORM_EPSILON = 1e-06
MESH = pl.DeviceIdType.MESH
VMEM = pltpu.VMEM
BF = jnp.bfloat16
F32 = jnp.float32
I16 = jnp.int16
TOP = 32767.0


def xor(me, r):
    out, bit = me, 1
    while bit <= r:
        if r & bit:
            out = out + bit * (1 - 2 * lax.rem(lax.div(me, bit), 2))
        bit *= 2
    return out


def greet(pairs):
    barrier = pltpu.get_barrier_semaphore()
    for axis, peer in pairs:
        pl.semaphore_signal(barrier, inc=1, device_id={axis: peer}, device_id_type=MESH)
    pl.semaphore_wait(barrier, len(pairs))


def nn(a, b):
    return jnp.dot(a, b, preferred_element_type=F32)


def nt(a, b):
    return lax.dot_general(a, b, (((1,), (1,)), ((), ())), preferred_element_type=F32)


def tn(a, b):
    return lax.dot_general(a, b, (((0,), (0,)), ((), ())), preferred_element_type=F32)


def eye(rows):
    return lax.broadcasted_iota(jnp.int32, (rows, rows), 0) == lax.broadcasted_iota(jnp.int32, (rows, rows), 1)


def to_lanes(column, diag):
    return jnp.sum(jnp.where(diag, column, 0.0), axis=0, keepdims=True)


def to_column(lanes, diag):
    return jnp.sum(jnp.where(diag, lanes, 0.0), axis=1, keepdims=True)


def coded(x, axis):
    peak = jnp.maximum(jnp.max(jnp.abs(x), axis=axis, keepdims=True), 1e-33)
    return jnp.round(x * (TOP / peak)).astype(jnp.int32).astype(I16), peak * (1.0 / TOP)


def decoded(x):
    return x.astype(jnp.int32).astype(F32)


class Post:
    def __init__(self, sems):
        self.sems, self.count, self.sent = sems, 0, []

    def __call__(self, src, dst, axis, peer):
        i = self.count
        self.count += 1
        cp = pltpu.make_async_remote_copy(
            src_ref=src, dst_ref=dst, send_sem=self.sems.at[0, i], recv_sem=self.sems.at[1, i],
            device_id={axis: peer}, device_id_type=MESH,
        )
        cp.start()
        self.sent.append(cp)
        return cp

    def finish(self):
        for cp in self.sent:
            cp.wait_send()


def packed_shape(rows, width):
    if width == 192 and rows % 64 == 0:
        return rows + rows // 2, 128
    return rows, width


def step_kernel(
    n, count, total, ih, th, ip, tp, pa, lg,
    oih, oth, wqi, wqt, ws, sc_out,
    xi, xt, iu, il, tu, tl, gi, temb, raw, lt, mx, cst, cb, rst, rb, wl,
    tq, ts, tqr, tsr, iup, crecv, iq, isc, iqr, isr, hx, hy, hxg, hyg, di, dt, dgi, dgt, ghi, ght,
    zqi, zqt, zqir, zqtr, zs, zsr, wpi, wpt, scz, scd, sems,
):
    b, d = lax.axis_index("branch"), lax.axis_index("dp")
    core, chip = lax.rem(d, 2), lax.div(d, 2)
    other = 1 - core
    chips = count // 2
    own, embed, width = ih.shape[1], ip.shape[2], tp.shape[1]
    rows, half = n * own, embed // 2
    mid = rows // 2
    ri, rt = ip.shape[1] // chips, width // chips
    packed = xt.shape[1] != rows
    post = Post(sems)
    diag = eye(own)
    zpeers = [xor(b, r) for r in range(n)]
    dpeers = [xor(d, m) for m in range(count)]
    far = list(range(n - 1, 0, -1))
    outward = list(range(2, count, 2))
    bits = [1 << k for k in range(n.bit_length() - 1)][::-1]

    if packed:
        xt[b, :rows] = th[:, :128]
        xt[b, rows:, :64] = th[:mid, 128:]
        xt[b, rows:, 64:] = th[mid:, 128:]
    else:
        xt[b] = th[...]
    greet([("branch", zpeers[r]) for r in range(1, n)] + [("dp", dpeers[m]) for m in range(1, count)])

    features = {r: post(ih.at[zpeers[r]], xi.at[b], "branch", zpeers[r]) for r in far}
    parts = 2
    prow = xt.shape[1] // parts
    tin = {}

    def text_send(r, m, k):
        piece = xt.at[zpeers[r], pl.ds(k * prow, prow)]
        tin[(r ^ m, k)] = post(piece, piece, "branch", zpeers[m])

    for m in bits:
        for k in range(parts):
            text_send(0, m, k)

    def arrive(r):
        for k in range(parts):
            tin[(r, k)].wait_recv()
            for m in bits:
                if m < (r & -r):
                    text_send(r, m, k)

    def normal(x):
        size = jnp.sqrt(jnp.sum(x * x, axis=1, keepdims=True) + NORM_EPSILON)
        return x / size, size

    def text_part(s):
        if packed:
            main, tail = xt[s, :rows], xt[s, rows:]
            low = tp[s, 128:, :]
            zero = jnp.zeros_like(low)
            y = nn(main, tp[s, :128, :])
            lo = nn(tail, jnp.concatenate([low, zero], axis=0))
            hi = nn(tail, jnp.concatenate([zero, low], axis=0))
            y = y + jnp.concatenate([lo, hi], axis=0)
        else:
            y = nn(xt[s], tp[s])
        return y.reshape(n, own, embed)

    raw[...] = text_part(b)
    xi[b] = ih[b]
    x = nn(ih[b], ip[b])
    for r in far[::-1]:
        features[r].wait_recv()
        x = x + nn(xi[zpeers[r]], ip[zpeers[r]])
    u, size = normal(x)
    iu[...] = u
    il[...] = jnp.broadcast_to(size, il.shape)
    gi[d] = u.astype(BF)
    gin = {m: post(gi.at[d], gi.at[d], "dp", dpeers[m]) for m in outward + [1]}

    arrival = sorted(range(1, n), key=lambda r: (r & 1, bin(r).count("1"), -r))
    for r in arrival:
        if r == 1:
            for m in outward:
                gin[m].wait_recv()
                piece = gi.at[dpeers[m]]
                gin[m ^ 1] = post(piece, piece, "dp", dpeers[1])
        arrive(r)
        raw[...] = raw[...] + text_part(zpeers[r])
    for t in range(n):
        u, _ = normal(raw[t])
        temb[t] = u.astype(BF)
    u, size = normal(raw[b])
    tu[...] = u
    tl[...] = jnp.broadcast_to(size, tl.shape)
    for m in range(1, count, 2):
        gin[m].wait_recv()

    def pair(q):
        return gi[2 * q : 2 * q + 2].reshape(2 * own, embed)

    scale = jnp.exp(lg[...])
    texts = temb[...].reshape(rows, embed)
    for q in range(chips):
        y = scale * nt(texts, pair(q))
        lt[q] = y.reshape(n, own, 2 * own)
        top = jnp.max(y, axis=0, keepdims=True)
        cst[0, q] = top
        cst[1, q] = jnp.sum(jnp.exp(y - top), axis=0, keepdims=True)
        near = jnp.maximum(y[:, :own], y[:, own:])
        mx[...] = near if q == 0 else jnp.maximum(mx[...], near)
    cin = [post(cst, cb.at[m], "dp", dpeers[m]) for m in range(1, count)]
    for t in range(n):
        top = jnp.max(mx[pl.ds(t * own, own)], axis=1, keepdims=True)
        mass = jnp.zeros((own, own), F32)
        for q in range(chips):
            e = jnp.exp(lt[q, t] - top)
            mass = mass + e[:, :own] + e[:, own:]
        rst[0, t] = to_lanes(top, diag)
        rst[1, t] = to_lanes(jnp.sum(mass, axis=1, keepdims=True), diag)
    rin = [post(rst, rb.at[r], "branch", zpeers[r]) for r in far]

    def turned(x):
        return jnp.transpose(x.astype(F32))

    start = pl.multiple_of(b * own, own)
    for s in range(n):
        h = turned(xi[s]).astype(BF)
        for q in range(chips):
            hx[q, s] = h[q * ri : (q + 1) * ri]
        h = turned(xt[s, pl.ds(start, own)])
        if packed:
            tail = turned(xt[s, pl.ds(pl.multiple_of(rows + lax.rem(b, n // 2) * own, own), own)])
            h = jnp.concatenate([h, jnp.where(b < n // 2, tail[:64], tail[64:])], axis=0)
        h = h.astype(BF)
        for q in range(chips):
            hy[q, s] = h[q * rt : (q + 1) * rt]
    hin = []
    for m in range(1, count):
        k = lax.div(dpeers[m], 2)
        hin.append(post(hx.at[k], hxg.at[d], "dp", dpeers[m]))
        hin.append(post(hy.at[k], hyg.at[d], "dp", dpeers[m]))
    hxg[d] = hx[chip]
    hyg[d] = hy[chip]

    def merged(held, came, k, many):
        top = held[0, k]
        for m in range(1, many):
            top = jnp.maximum(top, came[m, 0, k])
        mass = held[1, k] * jnp.exp(held[0, k] - top)
        for m in range(1, many):
            mass = mass + came[m, 1, k] * jnp.exp(came[m, 0, k] - top)
        return top + jnp.log(mass)

    for cp in cin:
        cp.wait_recv()
    ilse = [merged(cst, cb, q, count) for q in range(chips)]
    for cp in rin:
        cp.wait_recv()
    tlse = [merged(rst, rb, t, n) for t in range(n)]

    mine = jnp.zeros((1, own), F32)
    for q in range(chips):
        mine = mine + jnp.where(chip == q, jnp.where(core == 0, ilse[q][:, :own], ilse[q][:, own:]), 0.0)
    for t in range(n):
        mine = mine + jnp.where(b == t, tlse[t], 0.0)
    pos = jnp.zeros((own, 2 * own), F32)
    slope = jnp.zeros((own, 2 * own), F32)
    line = lax.broadcasted_iota(jnp.int32, (own, 2 * own), 0)
    inverse = 1.0 / (2.0 * total)
    for t in range(n):
        low = to_column(tlse[t], diag)
        ids = line + (d * rows + t * own)
        for q in range(chips):
            y = lt[q, t]
            want = jnp.concatenate([pa[2 * q * n + b], pa[(2 * q + 1) * n + b]], axis=1)
            hit = ids == want
            w = (jnp.exp(y - low) + jnp.exp(y - ilse[q]) - jnp.where(hit, 2.0, 0.0)) * inverse
            pos = pos + jnp.where(hit, y, 0.0)
            slope = slope + w * y
            wl[q, t] = w.astype(BF)

    def whole(x):
        return jnp.sum(jnp.sum(x, axis=0, keepdims=True), axis=1, keepdims=True)

    loss = (whole(mine) - 2.0 * whole(pos)) * inverse
    scz[b, 0:1] = jnp.broadcast_to(loss, (1, 128))
    scz[b, 1:2] = jnp.broadcast_to(whole(slope), (1, 128))

    def text_up(t):
        y = nn(wl[0, t], pair(0))
        for q in range(1, chips):
            y = y + nn(wl[q, t], pair(q))
        return y

    tback = []
    for r in far:
        y, s = coded(text_up(zpeers[r]), 1)
        tq[r] = y
        ts[r] = to_lanes(s, diag)
        tback.append((r, post(tq.at[r], tqr.at[r], "branch", zpeers[r]), post(ts.at[r], tsr.at[r], "branch", zpeers[r])))
    zin = [post(scz.at[b], scz.at[b], "branch", zpeers[r]) for r in far]
    couple = []
    turn = list(range(1, chips)) + [0]
    for m in turn:
        k = xor(chip, m)
        y = tn(wl[k].reshape(rows, 2 * own), texts)
        iup[0, k] = y[:own]
        iup[1, k] = y[own:]
        couple.append(post(iup.at[other, k], crecv.at[k], "dp", dpeers[1]))
    raw[0] = text_up(b)
    iback = []
    for m, cp in zip(turn, couple):
        k = xor(chip, m)
        cp.wait_recv()
        y = iup[core, k] + crecv[k]
        if m:
            y, s = coded(y, 1)
            iq[m] = y
            isc[m] = to_lanes(s, diag)
            iback.append((m, post(iq.at[m], iqr.at[m], "dp", dpeers[2 * m]), post(isc.at[m], isr.at[m], "dp", dpeers[2 * m])))
        else:
            raw[1] = y

    def lower(up, u, size):
        radial = jnp.sum(up * u, axis=1, keepdims=True)
        return ((up - u * radial) / size).astype(BF)

    def spread(low, held, gathered):
        held[0] = low[:, :half]
        held[1] = low[:, half:]
        got = {}
        for m in outward + list(range(1, count, 2)):
            piece = core if m % 2 == 0 else other
            got[m] = post(held.at[piece], gathered.at[d], "dp", dpeers[m])
        gathered[d] = held[core]
        return got

    def hidden(low, proj, held, out):
        got = []
        for r in far:
            k = zpeers[r]
            held[r] = nt(low, proj[k]).astype(BF)
            got.append(post(held.at[r], out.at[b], "branch", k))
        out[b] = nt(low, proj[b]).astype(BF)
        return got

    def combined(up, back, codes, lengths):
        for r, cp, cq in back:
            cp.wait_recv()
            cq.wait_recv()
            up = up + decoded(codes[r]) * to_column(lengths[r], diag)
        return up

    low = lower(scale * combined(raw[1], iback, iqr, isr), iu[...], il[:, 0:1])
    igot = spread(low, di, dgi)
    ends = hidden(low, ip, ghi, oih)
    for cp in hin:
        cp.wait_recv()
    low = lower(scale * combined(raw[0], tback, tqr, tsr), tu[...], tl[:, 0:1])
    tgot = spread(low, dt, dgt)
    ends = ends + hidden(low, tp, ght, oth)

    def product(held, got, gathered, size, out):
        y = nn(held[d].reshape(n * size, own), gathered[d])
        for m in outward + list(range(1, count, 2)):
            got[m].wait_recv()
            y = y + nn(held[dpeers[m]].reshape(n * size, own), gathered[dpeers[m]])
        out[...] = y.reshape(n, size, half)

    def exchange(part, wp, held, came):
        got = []
        for r in far:
            y, s = coded(wp[zpeers[r]], 0)
            held[r] = y
            zs[part, r] = s
            got.append((r, post(held.at[r], came.at[r], "branch", zpeers[r]),
                        post(zs.at[part, r], zsr.at[part, r], "branch", zpeers[r])))
        return got

    def settle(part, wp, came, got, out):
        y = wp[b]
        for r, cp, cq in got:
            cp.wait_recv()
            cq.wait_recv()
            y = y + decoded(came[r]) * zsr[part, r]
        y, s = coded(y, 0)
        out[d] = y
        ws[part, d] = s
        got = {}
        for m in outward + [1]:
            got[m] = (post(out.at[d], out.at[d], "dp", dpeers[m]),
                      post(ws.at[part, d], ws.at[part, d], "dp", dpeers[m]))
        return got

    def relay(part, got, out):
        for m in outward:
            k = dpeers[m]
            for cp in got[m]:
                cp.wait_recv()
            got[m ^ 1] = (post(out.at[k], out.at[k], "dp", dpeers[1]),
                          post(ws.at[part, k], ws.at[part, k], "dp", dpeers[1]))

    product(hxg, igot, dgi, ri, wpi)
    iz = exchange(0, wpi, zqi, zqir)
    product(hyg, tgot, dgt, rt, wpt)
    tz = exchange(1, wpt, zqt, zqtr)
    for cp in zin:
        cp.wait_recv()
    y = scz[0]
    for s in range(1, n):
        y = y + scz[s]
    scd[d] = y
    din = [post(scd.at[d], scd.at[d], "dp", dpeers[m]) for m in range(1, count)]
    ilast = settle(0, wpi, zqir, iz, wqi)
    tlast = settle(1, wpt, zqtr, tz, wqt)
    relay(0, ilast, wqi)
    relay(1, tlast, wqt)
    for cp in din + ends:
        cp.wait_recv()
    y = scd[0]
    for s in range(1, count):
        y = y + scd[s]
    sc_out[...] = y
    for last in (ilast, tlast):
        for m in range(1, count, 2):
            for cp in last[m]:
                cp.wait_recv()
    post.finish()


def per_device(image_hidden, text_hidden, image_proj, text_proj, log_inverse_sharpness, partner):
    n = lax.axis_size("branch")
    count = lax.axis_size("dp")
    chips = count // 2
    group, wide = image_hidden.shape
    thin = text_hidden.shape[1]
    own = group // n
    embed = image_proj.shape[1]
    half = embed // 2
    ri, rt = wide // chips, thin // chips
    total = group * count
    spec = pl.BlockSpec(memory_space=VMEM)
    prows, pwidth = packed_shape(group, thin)
    outs = [((n, own, wide), BF), ((n, own, thin), BF), ((count, ri, half), I16), ((count, rt, half), I16),
            ((2, count, 1, half), F32), ((2, 128), F32)]
    scratch = [
        VMEM((n, own, wide), BF), VMEM((n, prows, pwidth), BF),
        VMEM((own, embed), F32), VMEM((own, 128), F32), VMEM((own, embed), F32), VMEM((own, 128), F32),
        VMEM((count, own, embed), BF), VMEM((n, own, embed), BF), VMEM((n, own, embed), F32),
        VMEM((chips, n, own, 2 * own), F32), VMEM((group, own), F32),
        VMEM((2, chips, 1, 2 * own), F32), VMEM((count, 2, chips, 1, 2 * own), F32),
        VMEM((2, n, 1, own), F32), VMEM((n, 2, n, 1, own), F32), VMEM((chips, n, own, 2 * own), BF),
        VMEM((n, own, embed), I16), VMEM((n, 1, own), F32), VMEM((n, own, embed), I16), VMEM((n, 1, own), F32),
        VMEM((2, chips, own, embed), F32), VMEM((chips, own, embed), F32),
        VMEM((chips, own, embed), I16), VMEM((chips, 1, own), F32), VMEM((chips, own, embed), I16), VMEM((chips, 1, own), F32),
        VMEM((chips, n, ri, own), BF), VMEM((chips, n, rt, own), BF),
        VMEM((count, n, ri, own), BF), VMEM((count, n, rt, own), BF),
        VMEM((2, own, half), BF), VMEM((2, own, half), BF), VMEM((count, own, half), BF), VMEM((count, own, half), BF),
        VMEM((n, own, wide), BF), VMEM((n, own, thin), BF),
        VMEM((n, ri, half), I16), VMEM((n, rt, half), I16), VMEM((n, ri, half), I16), VMEM((n, rt, half), I16),
        VMEM((2, n, 1, half), F32), VMEM((2, n, 1, half), F32), VMEM((n, ri, half), F32), VMEM((n, rt, half), F32),
        VMEM((n, 2, 128), F32), VMEM((count, 2, 128), F32),
        pltpu.SemaphoreType.DMA((2, 24 * n + 24 * count)),
    ]
    args = (
        image_hidden.reshape(n, own, wide), text_hidden,
        image_proj.reshape(n, wide, embed), text_proj.reshape(n, thin, embed),
        partner.reshape(count * n, 1, own), log_inverse_sharpness.reshape(1, 1),
    )
    gih, gth, wqi, wqt, ws, sc = pl.pallas_call(
        functools.partial(step_kernel, n, count, total),
        out_shape=[jax.ShapeDtypeStruct(s, t) for s, t in outs],
        in_specs=[spec] * len(args),
        out_specs=[spec] * len(outs),
        scratch_shapes=scratch,
        compiler_params=pltpu.CompilerParams(
            collective_id=0, has_side_effects=True, vmem_limit_bytes=60 * 1024 * 1024
        ),
    )(*args)

    def joined(codes, lengths, size):
        y = codes.astype(F32) * lengths
        y = y.reshape(chips, 2, size, half).transpose(0, 2, 1, 3)
        return y.reshape(chips * size, embed)

    return (
        sc[0, :1],
        sc[1, :1],
        gih.reshape(group, wide),
        gth.reshape(group, thin),
        joined(wqi, ws[0], ri),
        joined(wqt, ws[1], rt),
    )


def solution(mesh):
    placed = (P("dp", "branch"), P("dp", "branch"), P(), P(), P(), P())
    return jax.shard_map(
        per_device,
        mesh=mesh,
        in_specs=placed,
        out_specs=(
            P(),
            P(),
            P("dp", "branch"),
            P("dp", "branch"),
            P("branch", None),
            P("branch", None),
        ),
        check_vma=False,
    )
```

```python
import functools

import jax
import jax.numpy as jnp
from jax import lax
from jax.experimental import pallas as pl
from jax.experimental.pallas import tpu as pltpu
from jax.sharding import PartitionSpec as P

NORM_EPSILON = 1e-06
MESH = pl.DeviceIdType.MESH
VMEM = pltpu.VMEM
BF = jnp.bfloat16
F32 = jnp.float32
I16 = jnp.int16
TOP = 32767.0


def xor(me, r):
    out, bit = me, 1
    while bit <= r:
        if r & bit:
            out = out + bit * (1 - 2 * lax.rem(lax.div(me, bit), 2))
        bit *= 2
    return out


def greet(pairs):
    barrier = pltpu.get_barrier_semaphore()
    for axis, peer in pairs:
        pl.semaphore_signal(barrier, inc=1, device_id={axis: peer}, device_id_type=MESH)
    pl.semaphore_wait(barrier, len(pairs))


def nn(a, b):
    return jnp.dot(a, b, preferred_element_type=F32)


def nt(a, b):
    return lax.dot_general(a, b, (((1,), (1,)), ((), ())), preferred_element_type=F32)


def tn(a, b):
    return lax.dot_general(a, b, (((0,), (0,)), ((), ())), preferred_element_type=F32)


def eye(rows, lanes):
    return lax.broadcasted_iota(jnp.int32, (rows, lanes), 0) == lax.broadcasted_iota(jnp.int32, (rows, lanes), 1)


def to_lanes(column, diag):
    return jnp.sum(jnp.where(diag, column, 0.0), axis=0, keepdims=True)


def to_column(lanes, diag):
    return jnp.sum(jnp.where(diag, lanes, 0.0), axis=1, keepdims=True)


def coded(x, axis):
    peak = jnp.maximum(jnp.max(jnp.abs(x), axis=axis, keepdims=True), 1e-33)
    return jnp.round(x * (TOP / peak)).astype(jnp.int32).astype(I16), peak * (1.0 / TOP)


def decoded(x):
    return x.astype(jnp.int32).astype(F32)


class Post:
    def __init__(self, sems):
        self.sems, self.count, self.sent = sems, 0, []

    def __call__(self, src, dst, axis, peer):
        i = self.count
        self.count += 1
        cp = pltpu.make_async_remote_copy(
            src_ref=src, dst_ref=dst, send_sem=self.sems.at[0, i], recv_sem=self.sems.at[1, i],
            device_id={axis: peer}, device_id_type=MESH,
        )
        cp.start()
        self.sent.append(cp)
        return cp

    def finish(self):
        for cp in self.sent:
            cp.wait_send()


def step_kernel(
    n, count, total, ih, th, ip, tp, pa, lg,
    oih, oth, wqi, wqt, wsi, wst, sc_out,
    xi, xt, iu, il, tu, tl, gi, temb, raw, lt, mx, cst, cb, rst, rb, wl,
    tq, ts, tqr, tsr, iup, crecv, iq, isc, iqr, isr, hx, hy, hxg, hyg, di, dt, dgi, dgt, ghi, ght,
    zqi, zqt, zqir, zqtr, zs, zsr, wpi, wpt, scz, scd, sems,
):
    b, d = lax.axis_index("branch"), lax.axis_index("dp")
    core, chip = lax.rem(d, 2), lax.div(d, 2)
    other = 1 - core
    chips = count // 2
    own, embed, width = ih.shape[1], ip.shape[2], tp.shape[1]
    rows, half = n * own, embed // 2
    hr = own // 2
    ri, rt = ip.shape[1] // chips, width // chips
    post = Post(sems)
    diag = eye(own, own)
    strip = eye(hr, own)
    odds = list(range(n - 1, 1, -2))
    evens = [r ^ 1 for r in odds]
    start = pl.multiple_of(b * own, own)
    column = pl.multiple_of(core * half, half)
    zpeers = [xor(b, r) for r in range(n)]
    dpeers = [xor(d, m) for m in range(count)]
    far = list(range(n - 1, 0, -1))
    outward = list(range(2, count, 2))
    bits = [1 << k for k in range(n.bit_length() - 1)][::-1]

    xt[b] = th[...]
    greet([("branch", zpeers[r]) for r in range(1, n)] + [("dp", dpeers[m]) for m in range(1, count)])

    features = {r: post(ih.at[zpeers[r]], xi.at[b], "branch", zpeers[r]) for r in far}
    parts = 2
    prow = xt.shape[1] // parts
    tin = {}

    def text_send(r, m, k):
        piece = xt.at[zpeers[r], pl.ds(k * prow, prow)]
        tin[(r ^ m, k)] = post(piece, piece, "branch", zpeers[m])

    for m in bits:
        for k in range(parts):
            text_send(0, m, k)

    def arrive(r):
        for k in range(parts):
            tin[(r, k)].wait_recv()
            for m in bits:
                if m < (r & -r):
                    text_send(r, m, k)

    def normal(x):
        size = jnp.sqrt(jnp.sum(x * x, axis=1, keepdims=True) + NORM_EPSILON)
        return x / size, size

    def text_part(s):
        return tn(xt[s], tp[s]).reshape(n, own, embed)

    raw[...] = text_part(b)
    xi[b] = ih[b]
    x = nn(ih[b], ip[b])
    for r in far[::-1]:
        features[r].wait_recv()
        x = x + nn(xi[zpeers[r]], ip[zpeers[r]])
    u, size = normal(x)
    iu[...] = u
    il[...] = jnp.broadcast_to(size, il.shape)
    gi[d] = u.astype(BF)
    gin = {m: post(gi.at[d], gi.at[d], "dp", dpeers[m]) for m in outward + [1]}

    arrival = sorted(range(1, n), key=lambda r: (r & 1, bin(r).count("1"), -r))
    for r in arrival:
        if r == 1:
            for m in outward:
                gin[m].wait_recv()
                piece = gi.at[dpeers[m]]
                gin[m ^ 1] = post(piece, piece, "dp", dpeers[1])
        arrive(r)
        raw[...] = raw[...] + text_part(zpeers[r])
    for t in range(n):
        u, _ = normal(raw[t])
        temb[t] = u.astype(BF)
    u, size = normal(raw[b])
    tu[...] = u
    tl[...] = jnp.broadcast_to(size, tl.shape)
    for m in range(1, count, 2):
        gin[m].wait_recv()

    def pair(q):
        return gi[2 * q : 2 * q + 2].reshape(2 * own, embed)

    scale = jnp.exp(lg[...])
    texts = temb[...].reshape(rows, embed)
    for q in range(chips):
        y = scale * nt(texts, pair(q))
        lt[q] = y.reshape(n, own, 2 * own)
        top = jnp.max(y, axis=0, keepdims=True)
        cst[0, q] = top
        cst[1, q] = jnp.sum(jnp.exp(y - top), axis=0, keepdims=True)
        near = jnp.maximum(y[:, :own], y[:, own:])
        mx[...] = near if q == 0 else jnp.maximum(mx[...], near)
    cin = [post(cst, cb.at[m], "dp", dpeers[m]) for m in range(1, count)]
    for t in range(n):
        top = jnp.max(mx[pl.ds(t * own, own)], axis=1, keepdims=True)
        mass = jnp.zeros((own, own), F32)
        for q in range(chips):
            e = jnp.exp(lt[q, t] - top)
            mass = mass + e[:, :own] + e[:, own:]
        rst[0, t] = to_lanes(top, diag)
        rst[1, t] = to_lanes(jnp.sum(mass, axis=1, keepdims=True), diag)
    rin = [post(rst, rb.at[r], "branch", zpeers[r]) for r in far]

    for s in range(n):
        h = jnp.transpose(xi[s].astype(F32)).astype(BF)
        for q in range(chips):
            hx[q, s] = h[q * ri : (q + 1) * ri]
        h = xt[s, :, pl.ds(start, own)]
        for q in range(chips):
            hy[q, s] = h[q * rt : (q + 1) * rt]
    hin = []
    for m in range(1, count):
        k = lax.div(dpeers[m], 2)
        hin.append(post(hx.at[k], hxg.at[d], "dp", dpeers[m]))
        hin.append(post(hy.at[k], hyg.at[d], "dp", dpeers[m]))
    hxg[d] = hx[chip]
    hyg[d] = hy[chip]

    def merged(held, came, k, many):
        top = held[0, k]
        for m in range(1, many):
            top = jnp.maximum(top, came[m, 0, k])
        mass = held[1, k] * jnp.exp(held[0, k] - top)
        for m in range(1, many):
            mass = mass + came[m, 1, k] * jnp.exp(came[m, 0, k] - top)
        return top + jnp.log(mass)

    for cp in cin:
        cp.wait_recv()
    ilse = [merged(cst, cb, q, count) for q in range(chips)]
    for cp in rin:
        cp.wait_recv()
    tlse = [merged(rst, rb, t, n) for t in range(n)]

    mine = jnp.zeros((1, own), F32)
    for q in range(chips):
        mine = mine + jnp.where(chip == q, jnp.where(core == 0, ilse[q][:, :own], ilse[q][:, own:]), 0.0)
    for t in range(n):
        mine = mine + jnp.where(b == t, tlse[t], 0.0)
    pos = jnp.zeros((own, 2 * own), F32)
    slope = jnp.zeros((own, 2 * own), F32)
    line = lax.broadcasted_iota(jnp.int32, (own, 2 * own), 0)
    inverse = 1.0 / (2.0 * total)
    for t in range(n):
        low = to_column(tlse[t], diag)
        ids = line + (d * rows + t * own)
        for q in range(chips):
            y = lt[q, t]
            want = jnp.concatenate([pa[2 * q * n + b], pa[(2 * q + 1) * n + b]], axis=1)
            hit = ids == want
            w = (jnp.exp(y - low) + jnp.exp(y - ilse[q]) - jnp.where(hit, 2.0, 0.0)) * inverse
            pos = pos + jnp.where(hit, y, 0.0)
            slope = slope + w * y
            wl[q, t] = w.astype(BF)

    def whole(x):
        return jnp.sum(jnp.sum(x, axis=0, keepdims=True), axis=1, keepdims=True)

    loss = (whole(mine) - 2.0 * whole(pos)) * inverse
    scz[b, 0:1] = jnp.broadcast_to(loss, (1, 128))
    scz[b, 1:2] = jnp.broadcast_to(whole(slope), (1, 128))

    def text_up(t):
        y = nn(wl[0, t], pair(0))
        for q in range(1, chips):
            y = y + nn(wl[q, t], pair(q))
        return y

    def text_post(r, h, y, peer):
        y, s = coded(y, 1)
        tq[r, h] = y
        ts[r, h] = to_lanes(s, strip)
        return (post(tq.at[r, h], tqr.at[r, h], "branch", peer), post(ts.at[r, h], tsr.at[r, h], "branch", peer))

    def text_take(r, h):
        for cp in tback[(r, h)]:
            cp.wait_recv()
        return decoded(tqr[r, h]) * to_column(tsr[r, h], strip)

    tback = {}
    for r in odds:
        y = text_up(zpeers[r])
        for h in (0, 1):
            tback[(r, h)] = text_post(r, h, y[h * hr : (h + 1) * hr], zpeers[1])
    raw[1] = text_up(zpeers[1])
    tback[(1, 0)] = text_post(1, 0, raw[1, :hr], zpeers[1])
    zin = [post(scz.at[b], scz.at[b], "branch", zpeers[r]) for r in far]
    couple = []
    turn = list(range(1, chips)) + [0]
    for m in turn:
        k = xor(chip, m)
        y = tn(wl[k].reshape(rows, 2 * own), texts)
        iup[0, k] = y[:own]
        iup[1, k] = y[own:]
        couple.append(post(iup.at[other, k], crecv.at[k], "dp", dpeers[1]))
    raw[0] = text_up(b)
    for e in evens:
        raw[e] = text_up(zpeers[e])

    def combine(h):
        for e in evens:
            y = raw[e, h * hr : (h + 1) * hr] + text_take(e ^ 1, h)
            tback[(e, h)] = text_post(e, h, y, zpeers[e])

    combine(0)
    tback[(1, 1)] = text_post(1, 1, raw[1, hr:], zpeers[1])
    iback = []
    for m, cp in zip(turn, couple):
        k = xor(chip, m)
        cp.wait_recv()
        y = iup[core, k] + crecv[k]
        if m:
            y, s = coded(y, 1)
            iq[m] = y
            isc[m] = to_lanes(s, diag)
            iback.append((m, post(iq.at[m], iqr.at[m], "dp", dpeers[2 * m]), post(isc.at[m], isr.at[m], "dp", dpeers[2 * m])))
        else:
            raw[1] = y
    combine(1)

    def lower(up, u, size):
        radial = jnp.sum(up * u, axis=1, keepdims=True)
        return ((up - u * radial) / size).astype(BF)

    def spread(low, held, gathered, first, got):
        size = low.shape[0]
        held[0, first : first + size] = low[:, :half]
        held[1, first : first + size] = low[:, half:]
        for m in outward + list(range(1, count, 2)):
            piece = core if m % 2 == 0 else other
            cp = post(held.at[piece, pl.ds(first, size)], gathered.at[d, pl.ds(first, size)], "dp", dpeers[m])
            got.setdefault(m, []).append(cp)
        gathered[d, first : first + size] = held[core, first : first + size]

    igot, tgot, ends = {}, {}, []

    def text_half(h):
        at = slice(h * hr, (h + 1) * hr)
        up = raw[0, at]
        for r in [1] + evens:
            up = up + text_take(r, h)
        spread(lower(scale * up, tu[at], tl[at, 0:1]), dt, dgt, h * hr, tgot)

    text_half(0)
    up = raw[1]
    for m, cp, cq in iback:
        cp.wait_recv()
        cq.wait_recv()
        up = up + decoded(iqr[m]) * to_column(isr[m], diag)
    low = lower(scale * up, iu[...], il[:, 0:1])
    spread(low, di, dgi, 0, igot)
    for r in far:
        k = zpeers[r]
        ghi[r] = nt(low, ip[k]).astype(BF)
        ends.append(post(ghi.at[r], oih.at[b], "branch", k))
    oih[b] = nt(low, ip[b]).astype(BF)
    for cp in hin:
        cp.wait_recv()
    text_half(1)
    low = jnp.concatenate([dt[0], dt[1]], axis=1)
    for r in far:
        k = zpeers[r]
        ght[r] = nt(tp[k], low).astype(BF)
        ends.append(post(ght.at[r], oth.at[:, pl.ds(start, own)], "branch", k))
    oth[:, pl.ds(start, own)] = nt(tp[b], low).astype(BF)

    def product(held, got, gathered, size, out):
        y = nn(held[d].reshape(n * size, own), gathered[d])
        for m in outward + list(range(1, count, 2)):
            for cp in got[m]:
                cp.wait_recv()
            y = y + nn(held[dpeers[m]].reshape(n * size, own), gathered[dpeers[m]])
        out[...] = y.reshape(n, size, half)

    def exchange(part, wp, held, came):
        got = []
        for r in far:
            y, s = coded(wp[zpeers[r]], 0)
            held[r] = y
            zs[part, r] = s
            got.append((r, post(held.at[r], came.at[r], "branch", zpeers[r]),
                        post(zs.at[part, r], zsr.at[part, r], "branch", zpeers[r])))
        return got

    def settle(part, wp, came, got, out):
        y = wp[b]
        for r, cp, cq in got:
            cp.wait_recv()
            cq.wait_recv()
            y = y + decoded(came[r]) * zsr[part, r]
        y, s = coded(y, 0)
        out[chip, :, pl.ds(column, half)] = y
        (wsi, wst)[part][chip, :, pl.ds(column, half)] = s
        got = {}
        for m in outward + [1]:
            got[m] = pass_on(part, chip, out, dpeers[m])
        return got

    def pass_on(part, k, out, peer):
        piece = out.at[k, :, pl.ds(column, half)]
        lengths = (wsi, wst)[part].at[k, :, pl.ds(column, half)]
        return (post(piece, piece, "dp", peer), post(lengths, lengths, "dp", peer))

    def relay(part, got, out):
        for m in outward:
            for cp in got[m]:
                cp.wait_recv()
            got[m ^ 1] = pass_on(part, xor(chip, m // 2), out, dpeers[1])

    product(hxg, igot, dgi, ri, wpi)
    iz = exchange(0, wpi, zqi, zqir)
    product(hyg, tgot, dgt, rt, wpt)
    tz = exchange(1, wpt, zqt, zqtr)
    for cp in zin:
        cp.wait_recv()
    y = scz[0]
    for s in range(1, n):
        y = y + scz[s]
    scd[d] = y
    din = [post(scd.at[d], scd.at[d], "dp", dpeers[m]) for m in range(1, count)]
    ilast = settle(0, wpi, zqir, iz, wqi)
    tlast = settle(1, wpt, zqtr, tz, wqt)
    relay(0, ilast, wqi)
    relay(1, tlast, wqt)
    for cp in din + ends:
        cp.wait_recv()
    y = scd[0]
    for s in range(1, count):
        y = y + scd[s]
    sc_out[...] = y
    for last in (ilast, tlast):
        for m in range(1, count, 2):
            for cp in last[m]:
                cp.wait_recv()
    post.finish()
    assert post.count == sems.shape[1]


def per_device(image_hidden, text_hidden, image_proj, text_proj, log_inverse_sharpness, partner):
    n = lax.axis_size("branch")
    count = lax.axis_size("dp")
    chips = count // 2
    group, wide = image_hidden.shape
    thin = text_hidden.shape[1]
    own = group // n
    embed = image_proj.shape[1]
    half = embed // 2
    ri, rt = wide // chips, thin // chips
    total = group * count
    spec = pl.BlockSpec(memory_space=VMEM)
    messages = 15 * (n - 1) + 12 * (count - 1) + 3 * chips - 2
    outs = [((n, own, wide), BF), ((thin, group), BF), ((chips, ri, embed), I16), ((chips, rt, embed), I16),
            ((chips, 1, embed), F32), ((chips, 1, embed), F32), ((2, 128), F32)]
    scratch = [
        VMEM((n, own, wide), BF), VMEM((n, thin, group), BF),
        VMEM((own, embed), F32), VMEM((own, 128), F32), VMEM((own, embed), F32), VMEM((own, 128), F32),
        VMEM((count, own, embed), BF), VMEM((n, own, embed), BF), VMEM((n, own, embed), F32),
        VMEM((chips, n, own, 2 * own), F32), VMEM((group, own), F32),
        VMEM((2, chips, 1, 2 * own), F32), VMEM((count, 2, chips, 1, 2 * own), F32),
        VMEM((2, n, 1, own), F32), VMEM((n, 2, n, 1, own), F32), VMEM((chips, n, own, 2 * own), BF),
        VMEM((n, 2, own // 2, embed), I16), VMEM((n, 2, 1, own), F32),
        VMEM((n, 2, own // 2, embed), I16), VMEM((n, 2, 1, own), F32),
        VMEM((2, chips, own, embed), F32), VMEM((chips, own, embed), F32),
        VMEM((chips, own, embed), I16), VMEM((chips, 1, own), F32), VMEM((chips, own, embed), I16), VMEM((chips, 1, own), F32),
        VMEM((chips, n, ri, own), BF), VMEM((chips, n, rt, own), BF),
        VMEM((count, n, ri, own), BF), VMEM((count, n, rt, own), BF),
        VMEM((2, own, half), BF), VMEM((2, own, half), BF), VMEM((count, own, half), BF), VMEM((count, own, half), BF),
        VMEM((n, own, wide), BF), VMEM((n, thin, own), BF),
        VMEM((n, ri, half), I16), VMEM((n, rt, half), I16), VMEM((n, ri, half), I16), VMEM((n, rt, half), I16),
        VMEM((2, n, 1, half), F32), VMEM((2, n, 1, half), F32), VMEM((n, ri, half), F32), VMEM((n, rt, half), F32),
        VMEM((n, 2, 128), F32), VMEM((count, 2, 128), F32),
        pltpu.SemaphoreType.DMA((2, messages)),
    ]
    args = (
        image_hidden.reshape(n, own, wide), text_hidden.T,
        image_proj.reshape(n, wide, embed), text_proj.reshape(n, thin, embed),
        partner.reshape(count * n, 1, own), log_inverse_sharpness.reshape(1, 1),
    )
    gih, gth, wqi, wqt, wsi, wst, sc = pl.pallas_call(
        functools.partial(step_kernel, n, count, total),
        out_shape=[jax.ShapeDtypeStruct(s, t) for s, t in outs],
        in_specs=[spec] * len(args),
        out_specs=[spec] * len(outs),
        scratch_shapes=scratch,
        compiler_params=pltpu.CompilerParams(
            collective_id=0, has_side_effects=True, vmem_limit_bytes=60 * 1024 * 1024
        ),
    )(*args)

    def joined(codes, lengths):
        return (codes.astype(F32) * lengths).reshape(-1, embed)

    return (
        sc[0, :1],
        sc[1, :1],
        gih.reshape(group, wide),
        gth.T,
        joined(wqi, wsi),
        joined(wqt, wst),
    )


def solution(mesh):
    placed = (P("dp", "branch"), P("dp", "branch"), P(), P(), P(), P())
    return jax.shard_map(
        per_device,
        mesh=mesh,
        in_specs=placed,
        out_specs=(
            P(),
            P(),
            P("dp", "branch"),
            P("dp", "branch"),
            P("branch", None),
            P("branch", None),
        ),
        check_vma=False,
    )
```

```python
import functools

import jax
import jax.numpy as jnp
from jax import lax
from jax.experimental import pallas as pl
from jax.experimental.pallas import tpu as pltpu
from jax.sharding import PartitionSpec as P

NORM_EPSILON = 1e-06
MESH = pl.DeviceIdType.MESH
VMEM = pltpu.VMEM
BF = jnp.bfloat16
F32 = jnp.float32
I16 = jnp.int16
TOP = 32767.0


def xor(me, r):
    out, bit = me, 1
    while bit <= r:
        if r & bit:
            out = out + bit * (1 - 2 * lax.rem(lax.div(me, bit), 2))
        bit *= 2
    return out


def greet(pairs):
    barrier = pltpu.get_barrier_semaphore()
    for axis, peer in pairs:
        pl.semaphore_signal(barrier, inc=1, device_id={axis: peer}, device_id_type=MESH)
    pl.semaphore_wait(barrier, len(pairs))


def nn(a, b):
    return jnp.dot(a, b, preferred_element_type=F32)


def nt(a, b):
    return lax.dot_general(a, b, (((1,), (1,)), ((), ())), preferred_element_type=F32)


def tn(a, b):
    return lax.dot_general(a, b, (((0,), (0,)), ((), ())), preferred_element_type=F32)


def eye(rows, lanes):
    return lax.broadcasted_iota(jnp.int32, (rows, lanes), 0) == lax.broadcasted_iota(jnp.int32, (rows, lanes), 1)


def to_lanes(column, diag):
    return jnp.sum(jnp.where(diag, column, 0.0), axis=0, keepdims=True)


def to_column(lanes, diag):
    return jnp.sum(jnp.where(diag, lanes, 0.0), axis=1, keepdims=True)


def coded(x, axis):
    peak = jnp.maximum(jnp.max(jnp.abs(x), axis=axis, keepdims=True), 1e-33)
    return jnp.round(x * (TOP / peak)).astype(jnp.int32).astype(I16), peak * (1.0 / TOP)


def decoded(x):
    return x.astype(jnp.int32).astype(F32)


class Post:
    def __init__(self, sems):
        self.sems, self.count, self.sent = sems, 0, []

    def __call__(self, src, dst, axis, peer):
        i = self.count
        self.count += 1
        cp = pltpu.make_async_remote_copy(
            src_ref=src, dst_ref=dst, send_sem=self.sems.at[0, i], recv_sem=self.sems.at[1, i],
            device_id={axis: peer}, device_id_type=MESH,
        )
        cp.start()
        self.sent.append(cp)
        return cp

    def finish(self):
        for cp in self.sent:
            cp.wait_send()


def step_kernel(
    n, count, total, ih, th, ip_in, tp_in, pa, lg,
    oih, oth, wqi, wqt, wsi, wst, sc_out,
    xi, xt, iu, il, tu, tl, gi, temb, raw, lt, mx, cst, cb, rst, rb, wl,
    tq, ts, tqr, tsr, iup, crecv, iq, isc, iqr, isr, hx, hy, hxg, hyg, di, dt, dgi, dgt, ghi, ght,
    zqi, zqt, zqir, zqtr, zs, zsr, wpi, wpt, scz, scd, ip, tp, loads, sems,
):
    b, d = lax.axis_index("branch"), lax.axis_index("dp")
    core, chip = lax.rem(d, 2), lax.div(d, 2)
    other = 1 - core
    chips = count // 2
    own, embed, width = ih.shape[1], ip.shape[2], tp.shape[1]
    rows, half = n * own, embed // 2
    hr = own // 2
    ri, rt = ip.shape[1] // chips, width // chips
    post = Post(sems)
    diag = eye(own, own)
    strip = eye(hr, own)
    odds = list(range(n - 1, 1, -2))
    evens = [r ^ 1 for r in odds]
    start = pl.multiple_of(b * own, own)
    column = pl.multiple_of(core * half, half)
    zpeers = [xor(b, r) for r in range(n)]
    dpeers = [xor(d, m) for m in range(count)]
    far = list(range(n - 1, 0, -1))
    outward = list(range(2, count, 2))
    bits = [1 << k for k in range(n.bit_length() - 1)][::-1]

    fetch = [pltpu.make_async_copy(ip_in, ip, loads.at[0]), pltpu.make_async_copy(tp_in, tp, loads.at[1])]
    for cp in fetch:
        cp.start()
    xt[b] = th[...]
    greet([("branch", zpeers[r]) for r in range(1, n)] + [("dp", dpeers[m]) for m in range(1, count)])

    features = {r: post(ih.at[zpeers[r]], xi.at[b], "branch", zpeers[r]) for r in far}
    parts = 2
    span = rows // parts
    per = n // parts
    tin = {}

    def text_send(r, m, k):
        piece = xt.at[zpeers[r], :, pl.ds(k * span, span)]
        tin[(r ^ m, k)] = post(piece, piece, "branch", zpeers[m])

    for k in range(parts):
        for m in bits:
            text_send(0, m, k)

    def arrive(r, k):
        tin[(r, k)].wait_recv()
        for m in bits:
            if m < (r & -r):
                text_send(r, m, k)

    def normal(x):
        size = jnp.sqrt(jnp.sum(x * x, axis=1, keepdims=True) + NORM_EPSILON)
        return x / size, size

    def text_part(s, k):
        return tn(xt[s, :, k * span : (k + 1) * span], tp[s]).reshape(per, own, embed)

    for cp in fetch:
        cp.wait()
    for k in range(parts):
        raw[k * per : (k + 1) * per] = text_part(b, k)
    xi[b] = ih[b]
    x = nn(ih[b], ip[b])
    for r in far[::-1]:
        features[r].wait_recv()
        x = x + nn(xi[zpeers[r]], ip[zpeers[r]])
    u, size = normal(x)
    iu[...] = u
    il[...] = jnp.broadcast_to(size, il.shape)
    gi[d] = u.astype(BF)
    gin = {m: post(gi.at[d], gi.at[d], "dp", dpeers[m]) for m in outward + [1]}

    def pieces(held, gathered):
        got = {}
        for m in outward + [1]:
            got[m] = post(held.at[xor(chip, m // 2)], gathered.at[d], "dp", dpeers[m])
        gathered[d] = held[chip]
        return got

    def hand_over(got, gathered):
        for m in outward:
            got[m].wait_recv()
            piece = gathered.at[dpeers[m]]
            got[m ^ 1] = post(piece, piece, "dp", dpeers[1])

    for s in range(n):
        h = jnp.transpose(xi[s].astype(F32)).astype(BF)
        for q in range(chips):
            hx[q, s] = h[q * ri : (q + 1) * ri]
    hin = pieces(hx, hxg)

    def pair(q):
        return gi[2 * q : 2 * q + 2].reshape(2 * own, embed)

    scale = jnp.exp(lg[...])

    def logits(k):
        texts = temb[k * per : (k + 1) * per].reshape(span, embed)
        for q in range(chips):
            y = scale * nt(texts, pair(q))
            lt[q, k * per : (k + 1) * per] = y.reshape(per, own, 2 * own)
            near = jnp.maximum(y[:, :own], y[:, own:])
            at = slice(k * span, (k + 1) * span)
            mx[at] = near if q == 0 else jnp.maximum(mx[at], near)
            top = jnp.max(y, axis=0, keepdims=True)
            mass = jnp.sum(jnp.exp(y - top), axis=0, keepdims=True)
            if k:
                old = cst[0, q]
                new = jnp.maximum(old, top)
                mass = mass * jnp.exp(top - new) + cst[1, q] * jnp.exp(old - new)
                top = new
            cst[0, q] = top
            cst[1, q] = mass

    arrival = sorted(range(1, n), key=lambda r: (r & 1, bin(r).count("1"), -r))
    for r in arrival:
        if r & 1 == 0:
            for k in range(parts):
                arrive(r, k)
            for k in range(parts):
                at = slice(k * per, (k + 1) * per)
                raw[at] = raw[at] + text_part(zpeers[r], k)
    hand_over(gin, gi)
    for k in range(parts):
        at = slice(k * per, (k + 1) * per)
        for r in arrival:
            if r & 1:
                arrive(r, k)
                raw[at] = raw[at] + text_part(zpeers[r], k)
        for t in range(k * per, (k + 1) * per):
            u, _ = normal(raw[t])
            temb[t] = u.astype(BF)
        if k == 0:
            hand_over(hin, hxg)
            for m in range(1, count, 2):
                gin[m].wait_recv()
        logits(k)
    u, size = normal(raw[b])
    tu[...] = u
    tl[...] = jnp.broadcast_to(size, tl.shape)
    texts = temb[...].reshape(rows, embed)
    cin = [post(cst, cb.at[m], "dp", dpeers[m]) for m in range(1, count)]
    for t in range(n):
        top = jnp.max(mx[pl.ds(t * own, own)], axis=1, keepdims=True)
        mass = jnp.zeros((own, own), F32)
        for q in range(chips):
            e = jnp.exp(lt[q, t] - top)
            mass = mass + e[:, :own] + e[:, own:]
        rst[0, t] = to_lanes(top, diag)
        rst[1, t] = to_lanes(jnp.sum(mass, axis=1, keepdims=True), diag)
    rin = [post(rst, rb.at[r], "branch", zpeers[r]) for r in far]

    for s in range(n):
        h = xt[s, :, pl.ds(start, own)]
        for q in range(chips):
            hy[q, s] = h[q * rt : (q + 1) * rt]
    yin = pieces(hy, hyg)

    def merged(held, came, k, many):
        top = held[0, k]
        for m in range(1, many):
            top = jnp.maximum(top, came[m, 0, k])
        mass = held[1, k] * jnp.exp(held[0, k] - top)
        for m in range(1, many):
            mass = mass + came[m, 1, k] * jnp.exp(came[m, 0, k] - top)
        return top + jnp.log(mass)

    for cp in cin:
        cp.wait_recv()
    ilse = [merged(cst, cb, q, count) for q in range(chips)]
    for cp in rin:
        cp.wait_recv()
    tlse = [merged(rst, rb, t, n) for t in range(n)]

    mine = jnp.zeros((1, own), F32)
    for q in range(chips):
        mine = mine + jnp.where(chip == q, jnp.where(core == 0, ilse[q][:, :own], ilse[q][:, own:]), 0.0)
    for t in range(n):
        mine = mine + jnp.where(b == t, tlse[t], 0.0)
    pos = jnp.zeros((own, 2 * own), F32)
    slope = jnp.zeros((own, 2 * own), F32)
    line = lax.broadcasted_iota(jnp.int32, (own, 2 * own), 0)
    inverse = 1.0 / (2.0 * total)
    for t in range(n):
        low = to_column(tlse[t], diag)
        ids = line + (d * rows + t * own)
        for q in range(chips):
            y = lt[q, t]
            want = jnp.concatenate([pa[2 * q * n + b], pa[(2 * q + 1) * n + b]], axis=1)
            hit = ids == want
            w = (jnp.exp(y - low) + jnp.exp(y - ilse[q]) - jnp.where(hit, 2.0, 0.0)) * inverse
            pos = pos + jnp.where(hit, y, 0.0)
            slope = slope + w * y
            wl[q, t] = w.astype(BF)

    def whole(x):
        return jnp.sum(jnp.sum(x, axis=0, keepdims=True), axis=1, keepdims=True)

    loss = (whole(mine) - 2.0 * whole(pos)) * inverse
    scz[b, 0:1] = jnp.broadcast_to(loss, (1, 128))
    scz[b, 1:2] = jnp.broadcast_to(whole(slope), (1, 128))

    def text_up(t):
        y = nn(wl[0, t], pair(0))
        for q in range(1, chips):
            y = y + nn(wl[q, t], pair(q))
        return y

    def text_post(r, h, y, peer):
        y, s = coded(y, 1)
        tq[r, h] = y
        ts[r, h] = to_lanes(s, strip)
        return (post(tq.at[r, h], tqr.at[r, h], "branch", peer), post(ts.at[r, h], tsr.at[r, h], "branch", peer))

    def text_take(r, h):
        for cp in tback[(r, h)]:
            cp.wait_recv()
        return decoded(tqr[r, h]) * to_column(tsr[r, h], strip)

    tback = {}
    for r in odds:
        y = text_up(zpeers[r])
        for h in (0, 1):
            tback[(r, h)] = text_post(r, h, y[h * hr : (h + 1) * hr], zpeers[1])
    raw[1] = text_up(zpeers[1])
    tback[(1, 0)] = text_post(1, 0, raw[1, :hr], zpeers[1])
    zin = [post(scz.at[b], scz.at[b], "branch", zpeers[r]) for r in far]
    couple = []
    turn = list(range(1, chips)) + [0]
    for m in turn:
        k = xor(chip, m)
        y = tn(wl[k].reshape(rows, 2 * own), texts)
        iup[0, k] = y[:own]
        iup[1, k] = y[own:]
        couple.append(post(iup.at[other, k], crecv.at[k], "dp", dpeers[1]))
    raw[0] = text_up(b)
    for e in evens:
        raw[e] = text_up(zpeers[e])

    def combine(h):
        for e in evens:
            y = raw[e, h * hr : (h + 1) * hr] + text_take(e ^ 1, h)
            tback[(e, h)] = text_post(e, h, y, zpeers[e])

    combine(0)
    hand_over(yin, hyg)
    tback[(1, 1)] = text_post(1, 1, raw[1, hr:], zpeers[1])
    iback = []
    for m, cp in zip(turn, couple):
        k = xor(chip, m)
        cp.wait_recv()
        y = iup[core, k] + crecv[k]
        if m:
            y, s = coded(y, 1)
            iq[m] = y
            isc[m] = to_lanes(s, diag)
            iback.append((m, post(iq.at[m], iqr.at[m], "dp", dpeers[2 * m]), post(isc.at[m], isr.at[m], "dp", dpeers[2 * m])))
        else:
            raw[1] = y
    combine(1)

    def lower(up, u, size):
        radial = jnp.sum(up * u, axis=1, keepdims=True)
        return ((up - u * radial) / size).astype(BF)

    def spread(low, held, gathered, first, got):
        size = low.shape[0]
        held[0, first : first + size] = low[:, :half]
        held[1, first : first + size] = low[:, half:]
        for m in outward + list(range(1, count, 2)):
            piece = core if m % 2 == 0 else other
            cp = post(held.at[piece, pl.ds(first, size)], gathered.at[d, pl.ds(first, size)], "dp", dpeers[m])
            got.setdefault(m, []).append(cp)
        gathered[d, first : first + size] = held[core, first : first + size]

    igot, tgot, ends = {}, {}, []

    def text_half(h):
        at = slice(h * hr, (h + 1) * hr)
        up = raw[0, at]
        for r in [1] + evens:
            up = up + text_take(r, h)
        spread(lower(scale * up, tu[at], tl[at, 0:1]), dt, dgt, h * hr, tgot)

    text_half(0)
    up = raw[1]
    for m, cp, cq in iback:
        cp.wait_recv()
        cq.wait_recv()
        up = up + decoded(iqr[m]) * to_column(isr[m], diag)
    low = lower(scale * up, iu[...], il[:, 0:1])
    spread(low, di, dgi, 0, igot)
    for r in far:
        k = zpeers[r]
        ghi[r] = nt(low, ip[k]).astype(BF)
        ends.append(post(ghi.at[r], oih.at[b], "branch", k))
    oih[b] = nt(low, ip[b]).astype(BF)
    for m in range(1, count, 2):
        hin[m].wait_recv()
        yin[m].wait_recv()
    text_half(1)
    low = jnp.concatenate([dt[0], dt[1]], axis=1)
    for r in far:
        k = zpeers[r]
        ght[r] = nt(tp[k], low).astype(BF)
        ends.append(post(ght.at[r], oth.at[:, pl.ds(start, own)], "branch", k))
    oth[:, pl.ds(start, own)] = nt(tp[b], low).astype(BF)

    def product(held, got, gathered, size, out):
        y = nn(held[d].reshape(n * size, own), gathered[d])
        for m in outward + list(range(1, count, 2)):
            for cp in got[m]:
                cp.wait_recv()
            y = y + nn(held[dpeers[m]].reshape(n * size, own), gathered[dpeers[m]])
        out[...] = y.reshape(n, size, half)

    def exchange(part, wp, held, came):
        got = []
        for r in far:
            y, s = coded(wp[zpeers[r]], 0)
            held[r] = y
            zs[part, r] = s
            got.append((r, post(held.at[r], came.at[r], "branch", zpeers[r]),
                        post(zs.at[part, r], zsr.at[part, r], "branch", zpeers[r])))
        return got

    def settle(part, wp, came, got, out):
        y = wp[b]
        for r, cp, cq in got:
            cp.wait_recv()
            cq.wait_recv()
            y = y + decoded(came[r]) * zsr[part, r]
        y, s = coded(y, 0)
        out[chip, :, pl.ds(column, half)] = y
        (wsi, wst)[part][chip, :, pl.ds(column, half)] = s
        got = {}
        for m in outward + [1]:
            got[m] = pass_on(part, chip, out, dpeers[m])
        return got

    def pass_on(part, k, out, peer):
        piece = out.at[k, :, pl.ds(column, half)]
        lengths = (wsi, wst)[part].at[k, :, pl.ds(column, half)]
        return (post(piece, piece, "dp", peer), post(lengths, lengths, "dp", peer))

    def relay(part, got, out):
        for m in outward:
            for cp in got[m]:
                cp.wait_recv()
            got[m ^ 1] = pass_on(part, xor(chip, m // 2), out, dpeers[1])

    product(hxg, igot, dgi, ri, wpi)
    iz = exchange(0, wpi, zqi, zqir)
    product(hyg, tgot, dgt, rt, wpt)
    tz = exchange(1, wpt, zqt, zqtr)
    for cp in zin:
        cp.wait_recv()
    y = scz[0]
    for s in range(1, n):
        y = y + scz[s]
    scd[d] = y
    din = [post(scd.at[d], scd.at[d], "dp", dpeers[m]) for m in range(1, count)]
    ilast = settle(0, wpi, zqir, iz, wqi)
    tlast = settle(1, wpt, zqtr, tz, wqt)
    relay(0, ilast, wqi)
    relay(1, tlast, wqt)
    for cp in din + ends:
        cp.wait_recv()
    y = scd[0]
    for s in range(1, count):
        y = y + scd[s]
    sc_out[...] = y
    for last in (ilast, tlast):
        for m in range(1, count, 2):
            for cp in last[m]:
                cp.wait_recv()
    post.finish()
    assert post.count == sems.shape[1]


def output_kernel(gih, gth, wqi, wqt, wsi, wst, sc, loss, slope, oih, oth, oi, ot):
    loss[...] = sc[0:1, 0:1]
    slope[...] = sc[1:2, 0:1]
    oih[...] = gih[...]
    oth[...] = gth[...]
    oi[...] = decoded(wqi[...]) * wsi[...]
    ot[...] = decoded(wqt[...]) * wst[...]


def per_device(image_hidden, text_hidden, image_proj, text_proj, log_inverse_sharpness, partner):
    n = lax.axis_size("branch")
    count = lax.axis_size("dp")
    chips = count // 2
    group, wide = image_hidden.shape
    thin = text_hidden.shape[1]
    own = group // n
    embed = image_proj.shape[1]
    half = embed // 2
    ri, rt = wide // chips, thin // chips
    total = group * count
    spec = pl.BlockSpec(memory_space=VMEM)
    messages = 15 * (n - 1) + 12 * (count - 1) + 3 * chips - 2
    outs = [((n, own, wide), BF), ((thin, group), BF), ((chips, ri, embed), I16), ((chips, rt, embed), I16),
            ((chips, 1, embed), F32), ((chips, 1, embed), F32), ((2, 128), F32)]
    scratch = [
        VMEM((n, own, wide), BF), VMEM((n, thin, group), BF),
        VMEM((own, embed), F32), VMEM((own, 128), F32), VMEM((own, embed), F32), VMEM((own, 128), F32),
        VMEM((count, own, embed), BF), VMEM((n, own, embed), BF), VMEM((n, own, embed), F32),
        VMEM((chips, n, own, 2 * own), F32), VMEM((group, own), F32),
        VMEM((2, chips, 1, 2 * own), F32), VMEM((count, 2, chips, 1, 2 * own), F32),
        VMEM((2, n, 1, own), F32), VMEM((n, 2, n, 1, own), F32), VMEM((chips, n, own, 2 * own), BF),
        VMEM((n, 2, own // 2, embed), I16), VMEM((n, 2, 1, own), F32),
        VMEM((n, 2, own // 2, embed), I16), VMEM((n, 2, 1, own), F32),
        VMEM((2, chips, own, embed), F32), VMEM((chips, own, embed), F32),
        VMEM((chips, own, embed), I16), VMEM((chips, 1, own), F32), VMEM((chips, own, embed), I16), VMEM((chips, 1, own), F32),
        VMEM((chips, n, ri, own), BF), VMEM((chips, n, rt, own), BF),
        VMEM((count, n, ri, own), BF), VMEM((count, n, rt, own), BF),
        VMEM((2, own, half), BF), VMEM((2, own, half), BF), VMEM((count, own, half), BF), VMEM((count, own, half), BF),
        VMEM((n, own, wide), BF), VMEM((n, thin, own), BF),
        VMEM((n, ri, half), I16), VMEM((n, rt, half), I16), VMEM((n, ri, half), I16), VMEM((n, rt, half), I16),
        VMEM((2, n, 1, half), F32), VMEM((2, n, 1, half), F32), VMEM((n, ri, half), F32), VMEM((n, rt, half), F32),
        VMEM((n, 2, 128), F32), VMEM((count, 2, 128), F32),
        VMEM((n, wide, embed), BF), VMEM((n, thin, embed), BF),
        pltpu.SemaphoreType.DMA((2,)), pltpu.SemaphoreType.DMA((2, messages)),
    ]
    args = (
        image_hidden.reshape(n, own, wide), text_hidden.T,
        image_proj.reshape(n, wide, embed), text_proj.reshape(n, thin, embed),
        partner.reshape(count * n, 1, own), log_inverse_sharpness.reshape(1, 1),
    )
    gih, gth, wqi, wqt, wsi, wst, sc = pl.pallas_call(
        functools.partial(step_kernel, n, count, total),
        out_shape=[jax.ShapeDtypeStruct(s, t) for s, t in outs],
        in_specs=[spec, spec, pl.BlockSpec(memory_space=pl.ANY), pl.BlockSpec(memory_space=pl.ANY), spec, spec],
        out_specs=[spec] * len(outs),
        scratch_shapes=scratch,
        compiler_params=pltpu.CompilerParams(
            collective_id=0, has_side_effects=True, vmem_limit_bytes=60 * 1024 * 1024
        ),
    )(*args)

    loss, slope, oih, oth, oi, ot = pl.pallas_call(
        output_kernel,
        out_shape=[
            jax.ShapeDtypeStruct((1, 1), F32), jax.ShapeDtypeStruct((1, 1), F32),
            jax.ShapeDtypeStruct((n, own, wide), BF), jax.ShapeDtypeStruct((thin, group), BF),
            jax.ShapeDtypeStruct((chips, ri, embed), F32), jax.ShapeDtypeStruct((chips, rt, embed), F32),
        ],
        in_specs=[spec] * 7,
        out_specs=[spec] * 6,
    )(gih, gth, wqi, wqt, wsi, wst, sc)
    return (
        loss.reshape(1),
        slope.reshape(1),
        oih.reshape(group, wide),
        oth.T,
        oi.reshape(wide, embed),
        ot.reshape(thin, embed),
    )


def solution(mesh):
    placed = (P("dp", "branch"), P("dp", "branch"), P(), P(), P(), P())
    return jax.shard_map(
        per_device,
        mesh=mesh,
        in_specs=placed,
        out_specs=(
            P(),
            P(),
            P("dp", "branch"),
            P("dp", "branch"),
            P("branch", None),
            P("branch", None),
        ),
        check_vma=False,
    )
```

```python
import functools

import jax
import jax.numpy as jnp
from jax import lax
from jax.experimental import pallas as pl
from jax.experimental.pallas import tpu as pltpu
from jax.sharding import PartitionSpec as P

NORM_EPSILON = 1e-06
MESH = pl.DeviceIdType.MESH
VMEM = pltpu.VMEM
BF = jnp.bfloat16
F32 = jnp.float32
I16 = jnp.int16
TOP = 32767.0


def xor(me, r):
    out, bit = me, 1
    while bit <= r:
        if r & bit:
            out = out + bit * (1 - 2 * lax.rem(lax.div(me, bit), 2))
        bit *= 2
    return out


def greet(pairs):
    barrier = pltpu.get_barrier_semaphore()
    for axis, peer in pairs:
        pl.semaphore_signal(barrier, inc=1, device_id={axis: peer}, device_id_type=MESH)
    pl.semaphore_wait(barrier, len(pairs))


def nn(a, b):
    return jnp.dot(a, b, preferred_element_type=F32)


def nt(a, b):
    return lax.dot_general(a, b, (((1,), (1,)), ((), ())), preferred_element_type=F32)


def tn(a, b):
    return lax.dot_general(a, b, (((0,), (0,)), ((), ())), preferred_element_type=F32)


def eye(rows, lanes):
    return lax.broadcasted_iota(jnp.int32, (rows, lanes), 0) == lax.broadcasted_iota(jnp.int32, (rows, lanes), 1)


def to_lanes(column, diag):
    return jnp.sum(jnp.where(diag, column, 0.0), axis=0, keepdims=True)


def to_column(lanes, diag):
    return jnp.sum(jnp.where(diag, lanes, 0.0), axis=1, keepdims=True)


def coded(x, axis):
    peak = jnp.maximum(jnp.max(jnp.abs(x), axis=axis, keepdims=True), 1e-33)
    return jnp.round(x * (TOP / peak)).astype(jnp.int32).astype(I16), peak * (1.0 / TOP)


def decoded(x):
    return x.astype(jnp.int32).astype(F32)


def ones(m):
    return bin(m).count("1")


class Post:
    def __init__(self, sems):
        self.sems, self.count, self.sent, self.taken = sems, 0, [], set()

    def __call__(self, src, dst, axis, peer):
        i = self.count
        self.count += 1
        cp = pltpu.make_async_remote_copy(
            src_ref=src, dst_ref=dst, send_sem=self.sems.at[0, i], recv_sem=self.sems.at[1, i],
            device_id={axis: peer}, device_id_type=MESH,
        )
        cp.start()
        self.sent.append(cp)
        return cp

    def take(self, cp):
        if id(cp) not in self.taken:
            self.taken.add(id(cp))
            cp.wait_recv()

    def finish(self):
        for cp in self.sent:
            cp.wait_send()


def step_kernel(
    n, count, total, ih, th, ip_in, tp_in, pa, lg,
    oih, oth, wqi, wqt, wsi, wst, sc_out,
    xi, xt, iu, il, tu, tl, gi, temb, raw, lt, mx, cst, cb, rst, rb, wl,
    tq, ts, tqr, tsr, iup, crecv, iq, isc, iqr, isr, hx, hy, hxg, hyg, di, dt, dgi, dgt, ghi, ght,
    zqi, zqt, zqir, zqtr, zs, zsr, wpi, wpt, scz, scd, ip, tp, loads, sems,
):
    b, d = lax.axis_index("branch"), lax.axis_index("dp")
    core, chip = lax.rem(d, 2), lax.div(d, 2)
    other = 1 - core
    chips = count // 2
    own, embed, width = ih.shape[1], ip.shape[2], tp.shape[1]
    rows, half = n * own, embed // 2
    hr = own // 2
    ri, rt = ip.shape[1] // chips, width // chips
    post = Post(sems)
    diag = eye(own, own)
    strip = eye(hr, own)
    odds = list(range(n - 1, 1, -2))
    evens = [r ^ 1 for r in odds]
    start = pl.multiple_of(b * own, own)
    column = pl.multiple_of(core * half, half)
    zpeers = [xor(b, r) for r in range(n)]
    dpeers = [xor(d, m) for m in range(count)]
    far = list(range(n - 1, 0, -1))
    outward = list(range(2, count, 2))
    bits = [1 << k for k in range(n.bit_length() - 1)][::-1]

    fetch = [pltpu.make_async_copy(ip_in, ip, loads.at[0]), pltpu.make_async_copy(tp_in, tp, loads.at[1])]
    for cp in fetch:
        cp.start()
    xt[b] = th[...]
    greet([("branch", zpeers[r]) for r in range(1, n)] + [("dp", dpeers[m]) for m in range(1, count)])

    features = {r: post(ih.at[zpeers[r]], xi.at[b], "branch", zpeers[r]) for r in far}
    parts = 2
    span = rows // parts
    per = n // parts
    tin = {}

    def text_send(r, m, k):
        piece = xt.at[zpeers[r], :, pl.ds(k * span, span)]
        tin[(r ^ m, k)] = post(piece, piece, "branch", zpeers[m])

    for k in range(parts):
        for m in bits:
            text_send(0, m, k)

    def arrive(r, k):
        tin[(r, k)].wait_recv()
        for m in bits:
            if m < (r & -r):
                text_send(r, m, k)

    def normal(x):
        size = jnp.sqrt(jnp.sum(x * x, axis=1, keepdims=True) + NORM_EPSILON)
        return x / size, size

    def text_part(s, k):
        return tn(xt[s, :, k * span : (k + 1) * span], tp[s]).reshape(per, own, embed)

    for cp in fetch:
        cp.wait()
    for k in range(parts):
        raw[k * per : (k + 1) * per] = text_part(b, k)
    xi[b] = ih[b]
    x = nn(ih[b], ip[b])
    for r in far[::-1]:
        features[r].wait_recv()
        x = x + nn(xi[zpeers[r]], ip[zpeers[r]])
    u, size = normal(x)
    iu[...] = u
    il[...] = jnp.broadcast_to(size, il.shape)
    gi[d] = u.astype(BF)
    gin = {m: post(gi.at[d], gi.at[d], "dp", dpeers[m]) for m in outward + [1]}

    def pieces(held, gathered):
        got = {}
        for m in outward + [1]:
            got[m] = post(held.at[xor(chip, m // 2)], gathered.at[d], "dp", dpeers[m])
        gathered[d] = held[chip]
        return got

    def hand_over(got, gathered):
        for m in outward:
            got[m].wait_recv()
            piece = gathered.at[dpeers[m]]
            got[m ^ 1] = post(piece, piece, "dp", dpeers[1])

    for s in range(n):
        h = jnp.transpose(xi[s].astype(F32)).astype(BF)
        for q in range(chips):
            hx[q, s] = h[q * ri : (q + 1) * ri]
    hin = pieces(hx, hxg)

    def pair(q):
        return gi[2 * q : 2 * q + 2].reshape(2 * own, embed)

    scale = jnp.exp(lg[...])

    def logits(k):
        texts = temb[k * per : (k + 1) * per].reshape(span, embed)
        for q in range(chips):
            y = scale * nt(texts, pair(q))
            lt[q, k * per : (k + 1) * per] = y.reshape(per, own, 2 * own)
            near = jnp.maximum(y[:, :own], y[:, own:])
            at = slice(k * span, (k + 1) * span)
            mx[at] = near if q == 0 else jnp.maximum(mx[at], near)
            top = jnp.max(y, axis=0, keepdims=True)
            mass = jnp.sum(jnp.exp(y - top), axis=0, keepdims=True)
            if k:
                old = cst[0, q]
                new = jnp.maximum(old, top)
                mass = mass * jnp.exp(top - new) + cst[1, q] * jnp.exp(old - new)
                top = new
            cst[0, q] = top
            cst[1, q] = mass

    arrival = sorted(range(1, n), key=lambda r: (r & 1, bin(r).count("1"), -r))
    for r in arrival:
        if r & 1 == 0:
            for k in range(parts):
                arrive(r, k)
            for k in range(parts):
                at = slice(k * per, (k + 1) * per)
                raw[at] = raw[at] + text_part(zpeers[r], k)
    hand_over(gin, gi)
    for k in range(parts):
        at = slice(k * per, (k + 1) * per)
        for r in arrival:
            if r & 1:
                arrive(r, k)
                raw[at] = raw[at] + text_part(zpeers[r], k)
        for t in range(k * per, (k + 1) * per):
            u, _ = normal(raw[t])
            temb[t] = u.astype(BF)
        if k == 0:
            hand_over(hin, hxg)
            for m in range(1, count, 2):
                gin[m].wait_recv()
        logits(k)
    u, size = normal(raw[b])
    tu[...] = u
    tl[...] = jnp.broadcast_to(size, tl.shape)
    texts = temb[...].reshape(rows, embed)
    cin = [post(cst, cb.at[m], "dp", dpeers[m]) for m in range(1, count)]
    for t in range(n):
        top = jnp.max(mx[pl.ds(t * own, own)], axis=1, keepdims=True)
        mass = jnp.zeros((own, own), F32)
        for q in range(chips):
            e = jnp.exp(lt[q, t] - top)
            mass = mass + e[:, :own] + e[:, own:]
        rst[0, t] = to_lanes(top, diag)
        rst[1, t] = to_lanes(jnp.sum(mass, axis=1, keepdims=True), diag)
    rin = [post(rst, rb.at[r], "branch", zpeers[r]) for r in far]

    for s in range(n):
        h = xt[s, :, pl.ds(start, own)]
        for q in range(chips):
            hy[q, s] = h[q * rt : (q + 1) * rt]
    yin = pieces(hy, hyg)

    def merged(held, came, k, many):
        top = held[0, k]
        for m in range(1, many):
            top = jnp.maximum(top, came[m, 0, k])
        mass = held[1, k] * jnp.exp(held[0, k] - top)
        for m in range(1, many):
            mass = mass + came[m, 1, k] * jnp.exp(came[m, 0, k] - top)
        return top + jnp.log(mass)

    for cp in cin:
        cp.wait_recv()
    ilse = [merged(cst, cb, q, count) for q in range(chips)]
    for cp in rin:
        cp.wait_recv()
    tlse = [merged(rst, rb, t, n) for t in range(n)]

    mine = jnp.zeros((1, own), F32)
    for q in range(chips):
        mine = mine + jnp.where(chip == q, jnp.where(core == 0, ilse[q][:, :own], ilse[q][:, own:]), 0.0)
    for t in range(n):
        mine = mine + jnp.where(b == t, tlse[t], 0.0)
    pos = jnp.zeros((own, 2 * own), F32)
    slope = jnp.zeros((own, 2 * own), F32)
    line = lax.broadcasted_iota(jnp.int32, (own, 2 * own), 0)
    inverse = 1.0 / (2.0 * total)
    for t in range(n):
        low = to_column(tlse[t], diag)
        ids = line + (d * rows + t * own)
        for q in range(chips):
            y = lt[q, t]
            want = jnp.concatenate([pa[2 * q * n + b], pa[(2 * q + 1) * n + b]], axis=1)
            hit = ids == want
            w = (jnp.exp(y - low) + jnp.exp(y - ilse[q]) - jnp.where(hit, 2.0, 0.0)) * inverse
            pos = pos + jnp.where(hit, y, 0.0)
            slope = slope + w * y
            wl[q, t] = w.astype(BF)

    def whole(x):
        return jnp.sum(jnp.sum(x, axis=0, keepdims=True), axis=1, keepdims=True)

    loss = (whole(mine) - 2.0 * whole(pos)) * inverse
    scz[b, 0:1] = jnp.broadcast_to(loss, (1, 128))
    scz[b, 1:2] = jnp.broadcast_to(whole(slope), (1, 128))

    def text_up(t):
        y = nn(wl[0, t], pair(0))
        for q in range(1, chips):
            y = y + nn(wl[q, t], pair(q))
        return y

    def text_post(r, h, y, peer):
        y, s = coded(y, 1)
        tq[r, h] = y
        ts[r, h] = to_lanes(s, strip)
        return (post(tq.at[r, h], tqr.at[r, h], "branch", peer), post(ts.at[r, h], tsr.at[r, h], "branch", peer))

    def text_take(r, h):
        for cp in tback[(r, h)]:
            cp.wait_recv()
        return decoded(tqr[r, h]) * to_column(tsr[r, h], strip)

    tback = {}
    for r in odds:
        y = text_up(zpeers[r])
        for h in (0, 1):
            tback[(r, h)] = text_post(r, h, y[h * hr : (h + 1) * hr], zpeers[1])
    raw[1] = text_up(zpeers[1])
    tback[(1, 0)] = text_post(1, 0, raw[1, :hr], zpeers[1])
    zin = [post(scz.at[b], scz.at[b], "branch", zpeers[r]) for r in far]
    couple = []
    turn = sorted(range(1, chips), key=lambda m: (ones(m) == 1, m)) + [0]
    near = [m for m in range(1, chips) if ones(m) == 1]
    for m in turn:
        k = xor(chip, m)
        y = tn(wl[k].reshape(rows, 2 * own), texts)
        iup[0, k] = y[:own]
        iup[1, k] = y[own:]
        couple.append(post(iup.at[other, k], crecv.at[k], "dp", dpeers[1]))
    raw[0] = text_up(b)
    for e in evens:
        raw[e] = text_up(zpeers[e])

    def combine(h):
        for e in evens:
            y = raw[e, h * hr : (h + 1) * hr] + text_take(e ^ 1, h)
            tback[(e, h)] = text_post(e, h, y, zpeers[e])

    combine(0)
    hand_over(yin, hyg)
    tback[(1, 1)] = text_post(1, 1, raw[1, hr:], zpeers[1])
    iback = {}

    def image_rows(m, h):
        return iup[core, xor(chip, m), h * hr : (h + 1) * hr]

    def image_post(m, h, y, via):
        y, s = coded(y, 1)
        iq[m, h] = y
        isc[m, h] = to_lanes(s, strip)
        iback[(m, h)] = (post(iq.at[m, h], iqr.at[m, h], "dp", dpeers[2 * via]),
                         post(isc.at[m, h], isr.at[m, h], "dp", dpeers[2 * via]))

    def image_take(m, h):
        for cp in iback[(m, h)]:
            cp.wait_recv()
        return decoded(iqr[m, h]) * to_column(isr[m, h], strip)

    def feeds(m, h):
        return [x for x in near if (x < m if h == 0 else x > m)]

    for m, cp in zip(turn, couple):
        k = xor(chip, m)
        cp.wait_recv()
        iup[core, k] = iup[core, k] + crecv[k]
        for h in (0, 1):
            if ones(m) == 2:
                image_post(m, h, image_rows(m, h), m & -m if h == 0 else m ^ (m & -m))
            elif ones(m) > 2 or (m and not feeds(m, h)):
                image_post(m, h, image_rows(m, h), m)
    combine(1)
    for m in near:
        for h in (0, 1):
            if feeds(m, h):
                y = image_rows(m, h)
                for x in feeds(m, h):
                    y = y + image_take(m | x, h)
                image_post(m, h, y, m)

    def lower(up, u, size):
        radial = jnp.sum(up * u, axis=1, keepdims=True)
        return ((up - u * radial) / size).astype(BF)

    def spread(low, held, gathered, first):
        size = low.shape[0]
        held[0, first : first + size] = low[:, :half]
        held[1, first : first + size] = low[:, half:]
        got = {}
        for m in outward:
            if ones(m) != 2:
                for c in (0, 1):
                    piece = held.at[core if c == 0 else other, pl.ds(first, size)]
                    got[m | c] = [post(piece, gathered.at[d, pl.ds(first, size)], "dp", dpeers[m | c])]
        piece = held.at[other, pl.ds(first, size)]
        got[1] = [post(piece, gathered.at[d, pl.ds(first, size)], "dp", dpeers[1])]
        gathered[d, first : first + size] = held[core, first : first + size]
        return got

    def spread_on(got, gathered, first, size):
        for c in (0, 1):
            for m in outward:
                if ones(m) == 2:
                    one = m & -m
                    for via, after, at in ((one, m ^ one, first), (m ^ one, one, first + size // 2)):
                        post.take(got[via | c][0])
                        piece = gathered.at[dpeers[via | c], pl.ds(at, size // 2)]
                        got.setdefault(m | c, []).append(post(piece, piece, "dp", dpeers[after]))

    ends = []

    def text_half(h):
        at = slice(h * hr, (h + 1) * hr)
        up = raw[0, at]
        for r in [1] + evens:
            up = up + text_take(r, h)
        return spread(lower(scale * up, tu[at], tl[at, 0:1]), dt, dgt, h * hr)

    tgot = [text_half(0)]
    halves = []
    for h in (0, 1):
        up = image_rows(0, h)
        for m in range(1, chips):
            if ones(m) != 2:
                up = up + image_take(m, h)
        halves.append(up)
    low = lower(scale * jnp.concatenate(halves, axis=0), iu[...], il[:, 0:1])
    igot = spread(low, di, dgi, 0)
    spread_on(tgot[0], dgt, 0, hr)
    for r in far:
        k = zpeers[r]
        ghi[r] = nt(low, ip[k]).astype(BF)
        ends.append(post(ghi.at[r], oih.at[b], "branch", k))
    oih[b] = nt(low, ip[b]).astype(BF)
    for m in range(1, count, 2):
        hin[m].wait_recv()
        yin[m].wait_recv()
    tgot.append(text_half(1))
    spread_on(igot, dgi, 0, own)
    low = jnp.concatenate([dt[0], dt[1]], axis=1)
    for r in far:
        k = zpeers[r]
        ght[r] = nt(tp[k], low).astype(BF)
        ends.append(post(ght.at[r], oth.at[:, pl.ds(start, own)], "branch", k))
    oth[:, pl.ds(start, own)] = nt(tp[b], low).astype(BF)
    spread_on(tgot[1], dgt, hr, hr)

    def product(held, got, gathered, size, out):
        y = nn(held[d].reshape(n * size, own), gathered[d])
        for m in outward + list(range(1, count, 2)):
            for part in got:
                for cp in part[m]:
                    post.take(cp)
            y = y + nn(held[dpeers[m]].reshape(n * size, own), gathered[dpeers[m]])
        out[...] = y.reshape(n, size, half)

    def exchange(part, wp, held, came):
        got = []
        for r in far:
            y, s = coded(wp[zpeers[r]], 0)
            held[r] = y
            zs[part, r] = s
            got.append((r, post(held.at[r], came.at[r], "branch", zpeers[r]),
                        post(zs.at[part, r], zsr.at[part, r], "branch", zpeers[r])))
        return got

    def settle(part, wp, came, got, out):
        y = wp[b]
        for r, cp, cq in got:
            cp.wait_recv()
            cq.wait_recv()
            y = y + decoded(came[r]) * zsr[part, r]
        y, s = coded(y, 0)
        out[chip, :, pl.ds(column, half)] = y
        (wsi, wst)[part][chip, :, pl.ds(column, half)] = s
        got = {}
        for m in outward + [1]:
            got[m] = pass_on(part, chip, out, dpeers[m])
        return got

    def pass_on(part, k, out, peer):
        piece = out.at[k, :, pl.ds(column, half)]
        lengths = (wsi, wst)[part].at[k, :, pl.ds(column, half)]
        return (post(piece, piece, "dp", peer), post(lengths, lengths, "dp", peer))

    def relay(part, got, out):
        for m in outward:
            for cp in got[m]:
                cp.wait_recv()
            got[m ^ 1] = pass_on(part, xor(chip, m // 2), out, dpeers[1])

    product(hxg, [igot], dgi, ri, wpi)
    iz = exchange(0, wpi, zqi, zqir)
    product(hyg, tgot, dgt, rt, wpt)
    tz = exchange(1, wpt, zqt, zqtr)
    for cp in zin:
        cp.wait_recv()
    y = scz[0]
    for s in range(1, n):
        y = y + scz[s]
    scd[d] = y
    din = [post(scd.at[d], scd.at[d], "dp", dpeers[m]) for m in range(1, count)]
    ilast = settle(0, wpi, zqir, iz, wqi)
    relay(0, ilast, wqi)
    tlast = settle(1, wpt, zqtr, tz, wqt)
    relay(1, tlast, wqt)
    for cp in din + ends:
        cp.wait_recv()
    y = scd[0]
    for s in range(1, count):
        y = y + scd[s]
    sc_out[...] = y
    for last in (ilast, tlast):
        for m in range(1, count, 2):
            for cp in last[m]:
                cp.wait_recv()
    post.finish()
    assert post.count == sems.shape[1]


def output_kernel(gih, gth, wqi, wqt, wsi, wst, sc, loss, slope, oih, oth, oi, ot):
    loss[...] = sc[0:1, 0:1]
    slope[...] = sc[1:2, 0:1]
    oih[...] = gih[...]
    oth[...] = gth[...]
    oi[...] = decoded(wqi[...]) * wsi[...]
    ot[...] = decoded(wqt[...]) * wst[...]


def per_device(image_hidden, text_hidden, image_proj, text_proj, log_inverse_sharpness, partner):
    n = lax.axis_size("branch")
    count = lax.axis_size("dp")
    chips = count // 2
    group, wide = image_hidden.shape
    thin = text_hidden.shape[1]
    own = group // n
    embed = image_proj.shape[1]
    half = embed // 2
    ri, rt = wide // chips, thin // chips
    total = group * count
    spec = pl.BlockSpec(memory_space=VMEM)
    twos = sum(ones(m) == 2 for m in range(chips))
    messages = 15 * (n - 1) + 12 * (count - 1) + 5 * chips - 4 + 6 * twos
    outs = [((n, own, wide), BF), ((thin, group), BF), ((chips, ri, embed), I16), ((chips, rt, embed), I16),
            ((chips, 1, embed), F32), ((chips, 1, embed), F32), ((2, 128), F32)]
    scratch = [
        VMEM((n, own, wide), BF), VMEM((n, thin, group), BF),
        VMEM((own, embed), F32), VMEM((own, 128), F32), VMEM((own, embed), F32), VMEM((own, 128), F32),
        VMEM((count, own, embed), BF), VMEM((n, own, embed), BF), VMEM((n, own, embed), F32),
        VMEM((chips, n, own, 2 * own), F32), VMEM((group, own), F32),
        VMEM((2, chips, 1, 2 * own), F32), VMEM((count, 2, chips, 1, 2 * own), F32),
        VMEM((2, n, 1, own), F32), VMEM((n, 2, n, 1, own), F32), VMEM((chips, n, own, 2 * own), BF),
        VMEM((n, 2, own // 2, embed), I16), VMEM((n, 2, 1, own), F32),
        VMEM((n, 2, own // 2, embed), I16), VMEM((n, 2, 1, own), F32),
        VMEM((2, chips, own, embed), F32), VMEM((chips, own, embed), F32),
        VMEM((chips, 2, own // 2, embed), I16), VMEM((chips, 2, 1, own), F32),
        VMEM((chips, 2, own // 2, embed), I16), VMEM((chips, 2, 1, own), F32),
        VMEM((chips, n, ri, own), BF), VMEM((chips, n, rt, own), BF),
        VMEM((count, n, ri, own), BF), VMEM((count, n, rt, own), BF),
        VMEM((2, own, half), BF), VMEM((2, own, half), BF), VMEM((count, own, half), BF), VMEM((count, own, half), BF),
        VMEM((n, own, wide), BF), VMEM((n, thin, own), BF),
        VMEM((n, ri, half), I16), VMEM((n, rt, half), I16), VMEM((n, ri, half), I16), VMEM((n, rt, half), I16),
        VMEM((2, n, 1, half), F32), VMEM((2, n, 1, half), F32), VMEM((n, ri, half), F32), VMEM((n, rt, half), F32),
        VMEM((n, 2, 128), F32), VMEM((count, 2, 128), F32),
        VMEM((n, wide, embed), BF), VMEM((n, thin, embed), BF),
        pltpu.SemaphoreType.DMA((2,)), pltpu.SemaphoreType.DMA((2, messages)),
    ]
    args = (
        image_hidden.reshape(n, own, wide), text_hidden.T,
        image_proj.reshape(n, wide, embed), text_proj.reshape(n, thin, embed),
        partner.reshape(count * n, 1, own), log_inverse_sharpness.reshape(1, 1),
    )
    gih, gth, wqi, wqt, wsi, wst, sc = pl.pallas_call(
        functools.partial(step_kernel, n, count, total),
        out_shape=[jax.ShapeDtypeStruct(s, t) for s, t in outs],
        in_specs=[spec, spec, pl.BlockSpec(memory_space=pl.ANY), pl.BlockSpec(memory_space=pl.ANY), spec, spec],
        out_specs=[spec] * len(outs),
        scratch_shapes=scratch,
        compiler_params=pltpu.CompilerParams(
            collective_id=0, has_side_effects=True, vmem_limit_bytes=60 * 1024 * 1024
        ),
    )(*args)

    loss, slope, oih, oth, oi, ot = pl.pallas_call(
        output_kernel,
        out_shape=[
            jax.ShapeDtypeStruct((1, 1), F32), jax.ShapeDtypeStruct((1, 1), F32),
            jax.ShapeDtypeStruct((n, own, wide), BF), jax.ShapeDtypeStruct((thin, group), BF),
            jax.ShapeDtypeStruct((chips, ri, embed), F32), jax.ShapeDtypeStruct((chips, rt, embed), F32),
        ],
        in_specs=[spec] * 7,
        out_specs=[spec] * 6,
    )(gih, gth, wqi, wqt, wsi, wst, sc)
    return (
        loss.reshape(1),
        slope.reshape(1),
        oih.reshape(group, wide),
        oth.T,
        oi.reshape(wide, embed),
        ot.reshape(thin, embed),
    )


def solution(mesh):
    placed = (P("dp", "branch"), P("dp", "branch"), P(), P(), P(), P())
    return jax.shard_map(
        per_device,
        mesh=mesh,
        in_specs=placed,
        out_specs=(
            P(),
            P(),
            P("dp", "branch"),
            P("dp", "branch"),
            P("branch", None),
            P("branch", None),
        ),
        check_vma=False,
    )
```

```python
import functools

import jax
import jax.numpy as jnp
from jax import lax
from jax.experimental import pallas as pl
from jax.experimental.pallas import tpu as pltpu
from jax.sharding import PartitionSpec as P

NORM_EPSILON = 1e-06
MESH = pl.DeviceIdType.MESH
VMEM = pltpu.VMEM
BF = jnp.bfloat16
F32 = jnp.float32
I16 = jnp.int16
TOP = 32767.0


def xor(me, r):
    out, bit = me, 1
    while bit <= r:
        if r & bit:
            out = out + bit * (1 - 2 * lax.rem(lax.div(me, bit), 2))
        bit *= 2
    return out


def greet(pairs):
    barrier = pltpu.get_barrier_semaphore()
    for axis, peer in pairs:
        pl.semaphore_signal(barrier, inc=1, device_id={axis: peer}, device_id_type=MESH)
    pl.semaphore_wait(barrier, len(pairs))


def nn(a, b):
    return jnp.dot(a, b, preferred_element_type=F32)


def nt(a, b):
    return lax.dot_general(a, b, (((1,), (1,)), ((), ())), preferred_element_type=F32)


def tn(a, b):
    return lax.dot_general(a, b, (((0,), (0,)), ((), ())), preferred_element_type=F32)


def eye(rows, lanes):
    return lax.broadcasted_iota(jnp.int32, (rows, lanes), 0) == lax.broadcasted_iota(jnp.int32, (rows, lanes), 1)


def to_lanes(column, diag):
    return jnp.sum(jnp.where(diag, column, 0.0), axis=0, keepdims=True)


def to_column(lanes, diag):
    return jnp.sum(jnp.where(diag, lanes, 0.0), axis=1, keepdims=True)


def coded(x, axis):
    peak = jnp.maximum(jnp.max(jnp.abs(x), axis=axis, keepdims=True), 1e-33)
    return jnp.round(x * (TOP / peak)).astype(jnp.int32).astype(I16), peak * (1.0 / TOP)


def decoded(x):
    return x.astype(jnp.int32).astype(F32)


class Lot:
    def __init__(self, post, span, both):
        self.post, self.span = post, span
        self.send = post.fresh()
        self.recv = post.fresh() if both else None
        post.lots.append(self)

    def wait(self, i):
        pltpu.make_async_copy(self.span, self.span, self.post.sems.at[i]).wait()

    def wait_recv(self):
        self.wait(self.recv)


class Post:
    def __init__(self, sems):
        self.sems, self.count, self.sent, self.lots = sems, 0, [], []

    def fresh(self):
        self.count += 1
        return self.count - 1

    def lot(self, span, both=False):
        return Lot(self, span, both)

    def __call__(self, src, dst, axis, peer, lot=None):
        send = self.fresh() if lot is None else lot.send
        recv = self.fresh() if lot is None or lot.recv is None else lot.recv
        cp = pltpu.make_async_remote_copy(
            src_ref=src, dst_ref=dst, send_sem=self.sems.at[send], recv_sem=self.sems.at[recv],
            device_id={axis: peer}, device_id_type=MESH,
        )
        cp.start()
        if lot is None:
            self.sent.append(cp)
        return cp

    def finish(self):
        for cp in self.sent:
            cp.wait_send()
        for lot in self.lots:
            lot.wait(lot.send)


def step_kernel(
    n, count, total, ih, th, ip_in, tp_in, pa, lg,
    oih, oth, wqi, wqt, wsi, wst, sc_out,
    xi, xt, iu, il, tu, tl, gi, temb, raw, lt, mx, cst, cb, rst, rb, wl,
    tq, ts, tqr, tsr, iup, crecv, iq, isc, iqr, isr, hx, hy, hxg, hyg, di, dt, dgi, dgt, ghi, ght,
    zqi, zqt, zqir, zqtr, zs, zsr, wpi, wpt, scz, scd, ip, tp, loads, sems,
):
    b, d = lax.axis_index("branch"), lax.axis_index("dp")
    core, chip = lax.rem(d, 2), lax.div(d, 2)
    other = 1 - core
    chips = count // 2
    own, embed, width = ih.shape[1], ip.shape[2], tp.shape[1]
    rows, half = n * own, embed // 2
    hr = own // 2
    ri, rt = ip.shape[1] // chips, width // chips
    post = Post(sems)
    diag = eye(own, own)
    strip = eye(hr, own)
    odds = list(range(n - 1, 1, -2))
    evens = [r ^ 1 for r in odds]
    start = pl.multiple_of(b * own, own)
    column = pl.multiple_of(core * half, half)
    zpeers = [xor(b, r) for r in range(n)]
    dpeers = [xor(d, m) for m in range(count)]
    far = list(range(n - 1, 0, -1))
    outward = list(range(2, count, 2))
    bits = [1 << k for k in range(n.bit_length() - 1)][::-1]

    fetch = [pltpu.make_async_copy(ip_in, ip, loads.at[0]), pltpu.make_async_copy(tp_in, tp, loads.at[1])]
    for cp in fetch:
        cp.start()
    xt[b] = th[...]
    greet([("branch", zpeers[r]) for r in range(1, n)] + [("dp", dpeers[m]) for m in range(1, count)])

    lot = post.lot(xi.at[: n - 1])
    features = {r: post(ih.at[zpeers[r]], xi.at[b], "branch", zpeers[r], lot) for r in far}
    text_lot = post.lot(xt.at[: n - 1])
    parts = 2
    span = rows // parts
    per = n // parts
    tin = {}

    def text_send(r, m, k):
        piece = xt.at[zpeers[r], :, pl.ds(k * span, span)]
        tin[(r ^ m, k)] = post(piece, piece, "branch", zpeers[m], text_lot)

    for k in range(parts):
        for m in bits:
            text_send(0, m, k)

    def arrive(r, k):
        tin[(r, k)].wait_recv()
        for m in bits:
            if m < (r & -r):
                text_send(r, m, k)

    def normal(x):
        size = jnp.sqrt(jnp.sum(x * x, axis=1, keepdims=True) + NORM_EPSILON)
        return x / size, size

    def text_part(s, k):
        return tn(xt[s, :, k * span : (k + 1) * span], tp[s]).reshape(per, own, embed)

    for cp in fetch:
        cp.wait()
    for k in range(parts):
        raw[k * per : (k + 1) * per] = text_part(b, k)
    xi[b] = ih[b]
    x = nn(ih[b], ip[b])
    for r in far[::-1]:
        features[r].wait_recv()
        x = x + nn(xi[zpeers[r]], ip[zpeers[r]])
    u, size = normal(x)
    iu[...] = u
    il[...] = jnp.broadcast_to(size, il.shape)
    gi[d] = u.astype(BF)
    gin_lot = post.lot(gi.at[: count - 1])
    gin = {m: post(gi.at[d], gi.at[d], "dp", dpeers[m], gin_lot) for m in outward + [1]}

    def pieces(held, gathered, lot):
        got = {}
        for m in outward + [1]:
            got[m] = post(held.at[xor(chip, m // 2)], gathered.at[d], "dp", dpeers[m], lot)
        gathered[d] = held[chip]
        return got

    def hand_over(got, gathered, lot):
        for m in outward:
            got[m].wait_recv()
            piece = gathered.at[dpeers[m]]
            got[m ^ 1] = post(piece, piece, "dp", dpeers[1], lot)

    for s in range(n):
        h = jnp.transpose(xi[s].astype(F32)).astype(BF)
        for q in range(chips):
            hx[q, s] = h[q * ri : (q + 1) * ri]
    hin_lot = post.lot(hxg.at[: count - 1])
    hin = pieces(hx, hxg, hin_lot)

    def pair(q):
        return gi[2 * q : 2 * q + 2].reshape(2 * own, embed)

    scale = jnp.exp(lg[...])

    def logits(k):
        texts = temb[k * per : (k + 1) * per].reshape(span, embed)
        for q in range(chips):
            y = scale * nt(texts, pair(q))
            lt[q, k * per : (k + 1) * per] = y.reshape(per, own, 2 * own)
            near = jnp.maximum(y[:, :own], y[:, own:])
            at = slice(k * span, (k + 1) * span)
            mx[at] = near if q == 0 else jnp.maximum(mx[at], near)
            top = jnp.max(y, axis=0, keepdims=True)
            mass = jnp.sum(jnp.exp(y - top), axis=0, keepdims=True)
            if k:
                old = cst[0, q]
                new = jnp.maximum(old, top)
                mass = mass * jnp.exp(top - new) + cst[1, q] * jnp.exp(old - new)
                top = new
            cst[0, q] = top
            cst[1, q] = mass

    arrival = sorted(range(1, n), key=lambda r: (r & 1, bin(r).count("1"), -r))
    for r in arrival:
        if r & 1 == 0:
            for k in range(parts):
                arrive(r, k)
            for k in range(parts):
                at = slice(k * per, (k + 1) * per)
                raw[at] = raw[at] + text_part(zpeers[r], k)
    hand_over(gin, gi, gin_lot)
    for k in range(parts):
        at = slice(k * per, (k + 1) * per)
        for r in arrival:
            if r & 1:
                arrive(r, k)
                raw[at] = raw[at] + text_part(zpeers[r], k)
        for t in range(k * per, (k + 1) * per):
            u, _ = normal(raw[t])
            temb[t] = u.astype(BF)
        if k == 0:
            hand_over(hin, hxg, hin_lot)
            for m in range(1, count, 2):
                gin[m].wait_recv()
        logits(k)
    u, size = normal(raw[b])
    tu[...] = u
    tl[...] = jnp.broadcast_to(size, tl.shape)
    texts = temb[...].reshape(rows, embed)
    cin = post.lot(cb.at[1:], True)
    for m in range(1, count):
        post(cst, cb.at[m], "dp", dpeers[m], cin)
    for t in range(n):
        top = jnp.max(mx[pl.ds(t * own, own)], axis=1, keepdims=True)
        mass = jnp.zeros((own, own), F32)
        for q in range(chips):
            e = jnp.exp(lt[q, t] - top)
            mass = mass + e[:, :own] + e[:, own:]
        rst[0, t] = to_lanes(top, diag)
        rst[1, t] = to_lanes(jnp.sum(mass, axis=1, keepdims=True), diag)
    rin = post.lot(rb.at[1:], True)
    for r in far:
        post(rst, rb.at[r], "branch", zpeers[r], rin)

    for s in range(n):
        h = xt[s, :, pl.ds(start, own)]
        for q in range(chips):
            hy[q, s] = h[q * rt : (q + 1) * rt]
    yin_lot = post.lot(hyg.at[: count - 1])
    yin = pieces(hy, hyg, yin_lot)

    def merged(held, came, k, many):
        top = held[0, k]
        for m in range(1, many):
            top = jnp.maximum(top, came[m, 0, k])
        mass = held[1, k] * jnp.exp(held[0, k] - top)
        for m in range(1, many):
            mass = mass + came[m, 1, k] * jnp.exp(came[m, 0, k] - top)
        return top + jnp.log(mass)

    cin.wait_recv()
    ilse = [merged(cst, cb, q, count) for q in range(chips)]
    rin.wait_recv()
    tlse = [merged(rst, rb, t, n) for t in range(n)]

    mine = jnp.zeros((1, own), F32)
    for q in range(chips):
        mine = mine + jnp.where(chip == q, jnp.where(core == 0, ilse[q][:, :own], ilse[q][:, own:]), 0.0)
    for t in range(n):
        mine = mine + jnp.where(b == t, tlse[t], 0.0)
    pos = jnp.zeros((own, 2 * own), F32)
    slope = jnp.zeros((own, 2 * own), F32)
    line = lax.broadcasted_iota(jnp.int32, (own, 2 * own), 0)
    inverse = 1.0 / (2.0 * total)
    for t in range(n):
        low = to_column(tlse[t], diag)
        ids = line + (d * rows + t * own)
        for q in range(chips):
            y = lt[q, t]
            want = jnp.concatenate([pa[2 * q * n + b], pa[(2 * q + 1) * n + b]], axis=1)
            hit = ids == want
            w = (jnp.exp(y - low) + jnp.exp(y - ilse[q]) - jnp.where(hit, 2.0, 0.0)) * inverse
            pos = pos + jnp.where(hit, y, 0.0)
            slope = slope + w * y
            wl[q, t] = w.astype(BF)

    def whole(x):
        return jnp.sum(jnp.sum(x, axis=0, keepdims=True), axis=1, keepdims=True)

    loss = (whole(mine) - 2.0 * whole(pos)) * inverse
    scz[b, 0:1] = jnp.broadcast_to(loss, (1, 128))
    scz[b, 1:2] = jnp.broadcast_to(whole(slope), (1, 128))

    def text_up(t):
        y = nn(wl[0, t], pair(0))
        for q in range(1, chips):
            y = y + nn(wl[q, t], pair(q))
        return y

    def text_post(r, h, y, peer):
        y, s = coded(y, 1)
        tq[r, h] = y
        ts[r, h] = to_lanes(s, strip)
        return (post(tq.at[r, h], tqr.at[r, h], "branch", peer), post(ts.at[r, h], tsr.at[r, h], "branch", peer))

    def text_take(r, h):
        for cp in tback[(r, h)]:
            cp.wait_recv()
        return decoded(tqr[r, h]) * to_column(tsr[r, h], strip)

    couple = []
    couple_lot = post.lot(crecv)
    turn = list(range(1, chips)) + [0]
    for m in turn:
        k = xor(chip, m)
        y = tn(wl[k].reshape(rows, 2 * own), texts)
        iup[0, k] = y[:own]
        iup[1, k] = y[own:]
        couple.append(post(iup.at[other, k], crecv.at[k], "dp", dpeers[1], couple_lot))
    tback = {}
    for r in odds:
        y = text_up(zpeers[r])
        for h in (0, 1):
            tback[(r, h)] = text_post(r, h, y[h * hr : (h + 1) * hr], zpeers[1])
    raw[1] = text_up(zpeers[1])
    tback[(1, 0)] = text_post(1, 0, raw[1, :hr], zpeers[1])
    zin = post.lot(scz.at[: n - 1], True)
    for r in far:
        post(scz.at[b], scz.at[b], "branch", zpeers[r], zin)
    iback = []
    for m, cp in zip(turn, couple):
        k = xor(chip, m)
        cp.wait_recv()
        y = iup[core, k] + crecv[k]
        if m:
            y, s = coded(y, 1)
            iq[m] = y
            isc[m] = to_lanes(s, diag)
            iback.append((m, post(iq.at[m], iqr.at[m], "dp", dpeers[2 * m]), post(isc.at[m], isr.at[m], "dp", dpeers[2 * m])))
        else:
            iup[core, k] = y
    for e in evens:
        raw[e] = text_up(zpeers[e])

    def combine(h):
        for e in evens:
            y = raw[e, h * hr : (h + 1) * hr] + text_take(e ^ 1, h)
            tback[(e, h)] = text_post(e, h, y, zpeers[e])

    combine(0)
    hand_over(yin, hyg, yin_lot)
    tback[(1, 1)] = text_post(1, 1, raw[1, hr:], zpeers[1])
    raw[0] = text_up(b)
    combine(1)

    def lower(up, u, size):
        radial = jnp.sum(up * u, axis=1, keepdims=True)
        return ((up - u * radial) / size).astype(BF)

    def spread(low, held, gathered, first, got, lot):
        size = low.shape[0]
        held[0, first : first + size] = low[:, :half]
        held[1, first : first + size] = low[:, half:]
        for m in outward + list(range(1, count, 2)):
            piece = core if m % 2 == 0 else other
            cp = post(held.at[piece, pl.ds(first, size)], gathered.at[d, pl.ds(first, size)], "dp", dpeers[m], lot)
            got.setdefault(m, []).append(cp)
        gathered[d, first : first + size] = held[core, first : first + size]

    igot, tgot = {}, {}
    igot_lot, tgot_lot = post.lot(dgi.at[: count - 1]), post.lot(dgt.at[: count - 1])
    ends = [post.lot(oih.at[: n - 1], True), post.lot(oth.at[:, : (n - 1) * own], True)]

    def text_half(h):
        at = slice(h * hr, (h + 1) * hr)
        up = raw[0, at]
        for r in [1] + evens:
            up = up + text_take(r, h)
        spread(lower(scale * up, tu[at], tl[at, 0:1]), dt, dgt, h * hr, tgot, tgot_lot)

    text_half(0)
    up = iup[core, chip]
    for m, cp, cq in iback:
        cp.wait_recv()
        cq.wait_recv()
        up = up + decoded(iqr[m]) * to_column(isr[m], diag)
    low = lower(scale * up, iu[...], il[:, 0:1])
    spread(low, di, dgi, 0, igot, igot_lot)
    for r in far:
        k = zpeers[r]
        ghi[r] = nt(low, ip[k]).astype(BF)
        post(ghi.at[r], oih.at[b], "branch", k, ends[0])
    oih[b] = nt(low, ip[b]).astype(BF)
    for m in range(1, count, 2):
        hin[m].wait_recv()
        yin[m].wait_recv()
    text_half(1)
    low = jnp.concatenate([dt[0], dt[1]], axis=1)
    for r in far:
        k = zpeers[r]
        ght[r] = nt(tp[k], low).astype(BF)
        post(ght.at[r], oth.at[:, pl.ds(start, own)], "branch", k, ends[1])
    oth[:, pl.ds(start, own)] = nt(tp[b], low).astype(BF)

    def product(held, got, gathered, size, out):
        y = nn(held[d].reshape(n * size, own), gathered[d])
        for m in outward + list(range(1, count, 2)):
            for cp in got[m]:
                cp.wait_recv()
            y = y + nn(held[dpeers[m]].reshape(n * size, own), gathered[dpeers[m]])
        out[...] = y.reshape(n, size, half)

    def exchange(part, wp, held, came):
        got = []
        for r in far:
            y, s = coded(wp[zpeers[r]], 0)
            held[r] = y
            zs[part, r] = s
            got.append((r, post(held.at[r], came.at[r], "branch", zpeers[r]),
                        post(zs.at[part, r], zsr.at[part, r], "branch", zpeers[r])))
        return got

    def settle(part, wp, came, got, out):
        y = wp[b]
        for r, cp, cq in got:
            cp.wait_recv()
            cq.wait_recv()
            y = y + decoded(came[r]) * zsr[part, r]
        y, s = coded(y, 0)
        out[chip, :, pl.ds(column, half)] = y
        (wsi, wst)[part][chip, :, pl.ds(column, half)] = s
        got = {}
        for m in outward + [1]:
            got[m] = pass_on(part, chip, out, dpeers[m])
        return got

    def pass_on(part, k, out, peer):
        piece = out.at[k, :, pl.ds(column, half)]
        lengths = (wsi, wst)[part].at[k, :, pl.ds(column, half)]
        return (post(piece, piece, "dp", peer), post(lengths, lengths, "dp", peer))

    def relay(part, got, out):
        for m in outward:
            for cp in got[m]:
                cp.wait_recv()
            got[m ^ 1] = pass_on(part, xor(chip, m // 2), out, dpeers[1])

    product(hxg, igot, dgi, ri, wpi)
    iz = exchange(0, wpi, zqi, zqir)
    product(hyg, tgot, dgt, rt, wpt)
    tz = exchange(1, wpt, zqt, zqtr)
    zin.wait_recv()
    y = scz[0]
    for s in range(1, n):
        y = y + scz[s]
    scd[d] = y
    din = post.lot(scd.at[: count - 1], True)
    for m in range(1, count):
        post(scd.at[d], scd.at[d], "dp", dpeers[m], din)
    ilast = settle(0, wpi, zqir, iz, wqi)
    relay(0, ilast, wqi)
    tlast = settle(1, wpt, zqtr, tz, wqt)
    relay(1, tlast, wqt)
    for lot in [din] + ends:
        lot.wait_recv()
    y = scd[0]
    for s in range(1, count):
        y = y + scd[s]
    sc_out[...] = y
    for last in (ilast, tlast):
        for m in range(1, count, 2):
            for cp in last[m]:
                cp.wait_recv()
    post.finish()
    assert post.count == sems.shape[0], (post.count, sems.shape)


def output_kernel(gih, gth, wqi, wqt, wsi, wst, sc, loss, slope, oih, oth, oi, ot):
    loss[...] = sc[0:1, 0:1]
    slope[...] = sc[1:2, 0:1]
    oih[...] = gih[...]
    oth[...] = gth[...]
    oi[...] = decoded(wqi[...]) * wsi[...]
    ot[...] = decoded(wqt[...]) * wst[...]


def per_device(image_hidden, text_hidden, image_proj, text_proj, log_inverse_sharpness, partner):
    n = lax.axis_size("branch")
    count = lax.axis_size("dp")
    chips = count // 2
    group, wide = image_hidden.shape
    thin = text_hidden.shape[1]
    own = group // n
    embed = image_proj.shape[1]
    half = embed // 2
    ri, rt = wide // chips, thin // chips
    total = group * count
    spec = pl.BlockSpec(memory_space=VMEM)
    messages = 20 + 19 * (n - 1) + 14 * (count - 1) + 5 * chips - 4
    outs = [((n, own, wide), BF), ((thin, group), BF), ((chips, ri, embed), I16), ((chips, rt, embed), I16),
            ((chips, 1, embed), F32), ((chips, 1, embed), F32), ((2, 128), F32)]
    scratch = [
        VMEM((n, own, wide), BF), VMEM((n, thin, group), BF),
        VMEM((own, embed), F32), VMEM((own, 128), F32), VMEM((own, embed), F32), VMEM((own, 128), F32),
        VMEM((count, own, embed), BF), VMEM((n, own, embed), BF), VMEM((n, own, embed), F32),
        VMEM((chips, n, own, 2 * own), F32), VMEM((group, own), F32),
        VMEM((2, chips, 1, 2 * own), F32), VMEM((count, 2, chips, 1, 2 * own), F32),
        VMEM((2, n, 1, own), F32), VMEM((n, 2, n, 1, own), F32), VMEM((chips, n, own, 2 * own), BF),
        VMEM((n, 2, own // 2, embed), I16), VMEM((n, 2, 1, own), F32),
        VMEM((n, 2, own // 2, embed), I16), VMEM((n, 2, 1, own), F32),
        VMEM((2, chips, own, embed), F32), VMEM((chips, own, embed), F32),
        VMEM((chips, own, embed), I16), VMEM((chips, 1, own), F32), VMEM((chips, own, embed), I16), VMEM((chips, 1, own), F32),
        VMEM((chips, n, ri, own), BF), VMEM((chips, n, rt, own), BF),
        VMEM((count, n, ri, own), BF), VMEM((count, n, rt, own), BF),
        VMEM((2, own, half), BF), VMEM((2, own, half), BF), VMEM((count, own, half), BF), VMEM((count, own, half), BF),
        VMEM((n, own, wide), BF), VMEM((n, thin, own), BF),
        VMEM((n, ri, half), I16), VMEM((n, rt, half), I16), VMEM((n, ri, half), I16), VMEM((n, rt, half), I16),
        VMEM((2, n, 1, half), F32), VMEM((2, n, 1, half), F32), VMEM((n, ri, half), F32), VMEM((n, rt, half), F32),
        VMEM((n, 2, 128), F32), VMEM((count, 2, 128), F32),
        VMEM((n, wide, embed), BF), VMEM((n, thin, embed), BF),
        pltpu.SemaphoreType.DMA((2,)), pltpu.SemaphoreType.DMA((messages,)),
    ]
    args = (
        image_hidden.reshape(n, own, wide), text_hidden.T,
        image_proj.reshape(n, wide, embed), text_proj.reshape(n, thin, embed),
        partner.reshape(count * n, 1, own), log_inverse_sharpness.reshape(1, 1),
    )
    gih, gth, wqi, wqt, wsi, wst, sc = pl.pallas_call(
        functools.partial(step_kernel, n, count, total),
        out_shape=[jax.ShapeDtypeStruct(s, t) for s, t in outs],
        in_specs=[spec, spec, pl.BlockSpec(memory_space=pl.ANY), pl.BlockSpec(memory_space=pl.ANY), spec, spec],
        out_specs=[spec] * len(outs),
        scratch_shapes=scratch,
        compiler_params=pltpu.CompilerParams(
            collective_id=0, has_side_effects=True, vmem_limit_bytes=60 * 1024 * 1024
        ),
    )(*args)

    loss, slope, oih, oth, oi, ot = pl.pallas_call(
        output_kernel,
        out_shape=[
            jax.ShapeDtypeStruct((1, 1), F32), jax.ShapeDtypeStruct((1, 1), F32),
            jax.ShapeDtypeStruct((n, own, wide), BF), jax.ShapeDtypeStruct((thin, group), BF),
            jax.ShapeDtypeStruct((chips, ri, embed), F32), jax.ShapeDtypeStruct((chips, rt, embed), F32),
        ],
        in_specs=[spec] * 7,
        out_specs=[spec] * 6,
    )(gih, gth, wqi, wqt, wsi, wst, sc)
    return (
        loss.reshape(1),
        slope.reshape(1),
        oih.reshape(group, wide),
        oth.T,
        oi.reshape(wide, embed),
        ot.reshape(thin, embed),
    )


def solution(mesh):
    placed = (P("dp", "branch"), P("dp", "branch"), P(), P(), P(), P())
    return jax.shard_map(
        per_device,
        mesh=mesh,
        in_specs=placed,
        out_specs=(
            P(),
            P(),
            P("dp", "branch"),
            P("dp", "branch"),
            P("branch", None),
            P("branch", None),
        ),
        check_vma=False,
    )
```

```python
import functools

import jax
import jax.numpy as jnp
from jax import lax
from jax.experimental import pallas as pl
from jax.experimental.pallas import tpu as pltpu
from jax.sharding import PartitionSpec as P

NORM_EPSILON = 1e-06
MESH = pl.DeviceIdType.MESH
VMEM = pltpu.VMEM
BF = jnp.bfloat16
F32 = jnp.float32
I16 = jnp.int16
TOP = 32767.0


def xor(me, r):
    out, bit = me, 1
    while bit <= r:
        if r & bit:
            out = out + bit * (1 - 2 * lax.rem(lax.div(me, bit), 2))
        bit *= 2
    return out


def greet(pairs):
    barrier = pltpu.get_barrier_semaphore()
    for axis, peer in pairs:
        pl.semaphore_signal(barrier, inc=1, device_id={axis: peer}, device_id_type=MESH)
    pl.semaphore_wait(barrier, len(pairs))


def nn(a, b):
    return jnp.dot(a, b, preferred_element_type=F32)


def nt(a, b):
    return lax.dot_general(a, b, (((1,), (1,)), ((), ())), preferred_element_type=F32)


def tn(a, b):
    return lax.dot_general(a, b, (((0,), (0,)), ((), ())), preferred_element_type=F32)


def eye(rows, lanes):
    return lax.broadcasted_iota(jnp.int32, (rows, lanes), 0) == lax.broadcasted_iota(jnp.int32, (rows, lanes), 1)


def to_lanes(column, diag):
    return jnp.sum(jnp.where(diag, column, 0.0), axis=0, keepdims=True)


def to_column(lanes, diag):
    return jnp.sum(jnp.where(diag, lanes, 0.0), axis=1, keepdims=True)


def coded(x, axis):
    peak = jnp.maximum(jnp.max(jnp.abs(x), axis=axis, keepdims=True), 1e-33)
    return jnp.round(x * (TOP / peak)).astype(jnp.int32).astype(I16), peak * (1.0 / TOP)


def decoded(x):
    return x.astype(jnp.int32).astype(F32)


class Lot:
    def __init__(self, post, span, both):
        self.post, self.span = post, span
        self.send = post.fresh()
        self.recv = post.fresh() if both else None
        post.lots.append(self)

    def wait(self, i):
        pltpu.make_async_copy(self.span, self.span, self.post.sems.at[i]).wait()

    def wait_recv(self):
        self.wait(self.recv)


class Post:
    def __init__(self, sems):
        self.sems, self.count, self.sent, self.lots = sems, 0, [], []

    def fresh(self):
        self.count += 1
        return self.count - 1

    def lot(self, span, both=False):
        return Lot(self, span, both)

    def __call__(self, src, dst, axis, peer, lot=None):
        send = self.fresh() if lot is None else lot.send
        recv = self.fresh() if lot is None or lot.recv is None else lot.recv
        cp = pltpu.make_async_remote_copy(
            src_ref=src, dst_ref=dst, send_sem=self.sems.at[send], recv_sem=self.sems.at[recv],
            device_id={axis: peer}, device_id_type=MESH,
        )
        cp.start()
        if lot is None:
            self.sent.append(cp)
        return cp

    def finish(self):
        for cp in self.sent:
            cp.wait_send()
        for lot in self.lots:
            lot.wait(lot.send)


def step_kernel(
    n, count, total, ih, th, ip_in, tp_in, pa, lg,
    oih, oth, wqi, wqt, wsi, wst, sc_out,
    xi, xt, iu, il, tu, tl, gi, temb, raw, lt, mx, cst, cb, rst, rb, wl,
    tq, ts, tqr, tsr, iup, crecv, iq, isc, iqr, isr, hx, hy, hxg, hyg, di, dt, dgi, dgt, ghi, ght,
    zqi, zqt, zqir, zqtr, zs, zsr, wpi, wpt, scz, scd, ip, tp, loads, sems,
):
    b, d = lax.axis_index("branch"), lax.axis_index("dp")
    core, chip = lax.rem(d, 2), lax.div(d, 2)
    other = 1 - core
    chips = count // 2
    own, embed, width = ih.shape[1], ip.shape[2], tp.shape[1]
    rows, half = n * own, embed // 2
    hr = own // 2
    ri, rt = ip.shape[1] // chips, width // chips
    post = Post(sems)
    diag = eye(own, own)
    strip = eye(hr, own)
    odds = list(range(n - 1, 1, -2))
    evens = [r ^ 1 for r in odds]
    start = pl.multiple_of(b * own, own)
    column = pl.multiple_of(core * half, half)
    zpeers = [xor(b, r) for r in range(n)]
    dpeers = [xor(d, m) for m in range(count)]
    far = list(range(n - 1, 0, -1))
    outward = sorted(range(2, count, 2), key=lambda m: -bin(m).count("1"))
    bits = [1 << k for k in range(n.bit_length() - 1)][::-1]

    fetch = [pltpu.make_async_copy(ip_in, ip, loads.at[0]), pltpu.make_async_copy(tp_in, tp, loads.at[1])]
    for cp in fetch:
        cp.start()
    xt[b] = th[...]
    greet([("branch", zpeers[r]) for r in range(1, n)] + [("dp", dpeers[m]) for m in range(1, count)])

    lot = post.lot(xi.at[: n - 1])
    features = {r: post(ih.at[zpeers[r]], xi.at[b], "branch", zpeers[r], lot) for r in far}
    text_lot = post.lot(xt.at[: n - 1])
    parts = 2
    span = rows // parts
    per = n // parts
    tin = {}

    def text_send(r, m, k):
        piece = xt.at[zpeers[r], :, pl.ds(k * span, span)]
        tin[(r ^ m, k)] = post(piece, piece, "branch", zpeers[m], text_lot)

    for k in range(parts):
        for m in bits:
            text_send(0, m, k)

    def arrive(r, k):
        tin[(r, k)].wait_recv()
        for m in bits:
            if m < (r & -r):
                text_send(r, m, k)

    def normal(x):
        size = jnp.sqrt(jnp.sum(x * x, axis=1, keepdims=True) + NORM_EPSILON)
        return x / size, size

    def text_part(s, k):
        return tn(xt[s, :, k * span : (k + 1) * span], tp[s]).reshape(per, own, embed)

    for cp in fetch:
        cp.wait()
    for k in range(parts):
        raw[k * per : (k + 1) * per] = text_part(b, k)
    xi[b] = ih[b]
    x = nn(ih[b], ip[b])
    for r in far[::-1]:
        features[r].wait_recv()
        x = x + nn(xi[zpeers[r]], ip[zpeers[r]])
    u, size = normal(x)
    iu[...] = u
    il[...] = jnp.broadcast_to(size, il.shape)
    gi[d] = u.astype(BF)
    gin_lot = post.lot(gi.at[: count - 1])
    gin = {m: post(gi.at[d], gi.at[d], "dp", dpeers[m], gin_lot) for m in outward + [1]}

    def pieces(held, gathered, lot):
        got = {}
        for m in outward + [1]:
            got[m] = post(held.at[xor(chip, m // 2)], gathered.at[d], "dp", dpeers[m], lot)
        gathered[d] = held[chip]
        return got

    def hand_over(got, gathered, lot):
        for m in outward:
            got[m].wait_recv()
            piece = gathered.at[dpeers[m]]
            got[m ^ 1] = post(piece, piece, "dp", dpeers[1], lot)

    for s in range(n):
        h = jnp.transpose(xi[s].astype(F32)).astype(BF)
        for q in range(chips):
            hx[q, s] = h[q * ri : (q + 1) * ri]
    hin_lot = post.lot(hxg.at[: count - 1])
    hin = pieces(hx, hxg, hin_lot)

    def pair(q):
        return gi[2 * q : 2 * q + 2].reshape(2 * own, embed)

    scale = jnp.exp(lg[...])

    def logits(k):
        texts = temb[k * per : (k + 1) * per].reshape(span, embed)
        for q in range(chips):
            y = scale * nt(texts, pair(q))
            lt[q, k * per : (k + 1) * per] = y.reshape(per, own, 2 * own)
            near = jnp.maximum(y[:, :own], y[:, own:])
            at = slice(k * span, (k + 1) * span)
            mx[at] = near if q == 0 else jnp.maximum(mx[at], near)
            top = jnp.max(y, axis=0, keepdims=True)
            mass = jnp.sum(jnp.exp(y - top), axis=0, keepdims=True)
            if k:
                old = cst[0, q]
                new = jnp.maximum(old, top)
                mass = mass * jnp.exp(top - new) + cst[1, q] * jnp.exp(old - new)
                top = new
            cst[0, q] = top
            cst[1, q] = mass

    arrival = sorted(range(1, n), key=lambda r: (r & 1, bin(r).count("1"), -r))
    for r in arrival:
        if r & 1 == 0:
            for k in range(parts):
                arrive(r, k)
            for k in range(parts):
                at = slice(k * per, (k + 1) * per)
                raw[at] = raw[at] + text_part(zpeers[r], k)
    hand_over(gin, gi, gin_lot)
    for k in range(parts):
        at = slice(k * per, (k + 1) * per)
        for r in arrival:
            if r & 1:
                arrive(r, k)
                raw[at] = raw[at] + text_part(zpeers[r], k)
        for t in range(k * per, (k + 1) * per):
            u, _ = normal(raw[t])
            temb[t] = u.astype(BF)
        if k == 0:
            hand_over(hin, hxg, hin_lot)
            for m in range(1, count, 2):
                gin[m].wait_recv()
        logits(k)
    u, size = normal(raw[b])
    tu[...] = u
    tl[...] = jnp.broadcast_to(size, tl.shape)
    texts = temb[...].reshape(rows, embed)
    cin = post.lot(cb.at[1:], True)
    for m in range(1, count):
        post(cst, cb.at[m], "dp", dpeers[m], cin)
    for t in range(n):
        top = jnp.max(mx[pl.ds(t * own, own)], axis=1, keepdims=True)
        mass = jnp.zeros((own, own), F32)
        for q in range(chips):
            e = jnp.exp(lt[q, t] - top)
            mass = mass + e[:, :own] + e[:, own:]
        rst[0, t] = to_lanes(top, diag)
        rst[1, t] = to_lanes(jnp.sum(mass, axis=1, keepdims=True), diag)
    rin = post.lot(rb.at[1:], True)
    for r in far:
        post(rst, rb.at[r], "branch", zpeers[r], rin)

    for s in range(n):
        h = xt[s, :, pl.ds(start, own)]
        for q in range(chips):
            hy[q, s] = h[q * rt : (q + 1) * rt]
    yin_lot = post.lot(hyg.at[: count - 1])
    yin = pieces(hy, hyg, yin_lot)

    def merged(held, came, k, many):
        top = held[0, k]
        for m in range(1, many):
            top = jnp.maximum(top, came[m, 0, k])
        mass = held[1, k] * jnp.exp(held[0, k] - top)
        for m in range(1, many):
            mass = mass + came[m, 1, k] * jnp.exp(came[m, 0, k] - top)
        return top + jnp.log(mass)

    cin.wait_recv()
    ilse = [merged(cst, cb, q, count) for q in range(chips)]
    rin.wait_recv()
    tlse = [merged(rst, rb, t, n) for t in range(n)]

    mine = jnp.zeros((1, own), F32)
    for q in range(chips):
        mine = mine + jnp.where(chip == q, jnp.where(core == 0, ilse[q][:, :own], ilse[q][:, own:]), 0.0)
    for t in range(n):
        mine = mine + jnp.where(b == t, tlse[t], 0.0)
    pos = jnp.zeros((own, 2 * own), F32)
    slope = jnp.zeros((own, 2 * own), F32)
    line = lax.broadcasted_iota(jnp.int32, (own, 2 * own), 0)
    inverse = 1.0 / (2.0 * total)
    for t in range(n):
        low = to_column(tlse[t], diag)
        ids = line + (d * rows + t * own)
        for q in range(chips):
            y = lt[q, t]
            want = jnp.concatenate([pa[2 * q * n + b], pa[(2 * q + 1) * n + b]], axis=1)
            hit = ids == want
            w = (jnp.exp(y - low) + jnp.exp(y - ilse[q]) - jnp.where(hit, 2.0, 0.0)) * inverse
            pos = pos + jnp.where(hit, y, 0.0)
            slope = slope + w * y
            wl[q, t] = w.astype(BF)

    def whole(x):
        return jnp.sum(jnp.sum(x, axis=0, keepdims=True), axis=1, keepdims=True)

    loss = (whole(mine) - 2.0 * whole(pos)) * inverse
    scz[b, 0:1] = jnp.broadcast_to(loss, (1, 128))
    scz[b, 1:2] = jnp.broadcast_to(whole(slope), (1, 128))

    def text_up(t):
        y = nn(wl[0, t], pair(0))
        for q in range(1, chips):
            y = y + nn(wl[q, t], pair(q))
        return y

    def text_post(r, h, y, peer):
        y, s = coded(y, 1)
        tq[r, h] = y
        ts[r, h] = to_lanes(s, strip)
        return (post(tq.at[r, h], tqr.at[r, h], "branch", peer), post(ts.at[r, h], tsr.at[r, h], "branch", peer))

    def text_take(r, h):
        for cp in tback[(r, h)]:
            cp.wait_recv()
        return decoded(tqr[r, h]) * to_column(tsr[r, h], strip)

    couple = []
    couple_lot = post.lot(crecv)
    turn = [m // 2 for m in outward] + [0]
    for m in turn:
        k = xor(chip, m)
        y = tn(wl[k].reshape(rows, 2 * own), texts)
        iup[0, k] = y[:own]
        iup[1, k] = y[own:]
        couple.append(post(iup.at[other, k], crecv.at[k], "dp", dpeers[1], couple_lot))
    tback = {}
    for r in odds:
        y = text_up(zpeers[r])
        for h in (0, 1):
            tback[(r, h)] = text_post(r, h, y[h * hr : (h + 1) * hr], zpeers[1])
    raw[1] = text_up(zpeers[1])
    tback[(1, 0)] = text_post(1, 0, raw[1, :hr], zpeers[1])
    zin = post.lot(scz.at[: n - 1], True)
    for r in far:
        post(scz.at[b], scz.at[b], "branch", zpeers[r], zin)
    iback = []
    for m, cp in zip(turn, couple):
        k = xor(chip, m)
        cp.wait_recv()
        y = iup[core, k] + crecv[k]
        if m:
            y, s = coded(y, 1)
            iq[m] = y
            isc[m] = to_lanes(s, diag)
            iback.append((m, post(iq.at[m], iqr.at[m], "dp", dpeers[2 * m]), post(isc.at[m], isr.at[m], "dp", dpeers[2 * m])))
        else:
            iup[core, k] = y
    for e in evens:
        raw[e] = text_up(zpeers[e])

    def combine(h):
        for e in evens:
            y = raw[e, h * hr : (h + 1) * hr] + text_take(e ^ 1, h)
            tback[(e, h)] = text_post(e, h, y, zpeers[e])

    combine(0)
    hand_over(yin, hyg, yin_lot)
    tback[(1, 1)] = text_post(1, 1, raw[1, hr:], zpeers[1])
    raw[0] = text_up(b)
    combine(1)

    def lower(up, u, size):
        radial = jnp.sum(up * u, axis=1, keepdims=True)
        return ((up - u * radial) / size).astype(BF)

    def spread(low, held, gathered, first, got, lot):
        size = low.shape[0]
        held[0, first : first + size] = low[:, :half]
        held[1, first : first + size] = low[:, half:]
        for m in outward + list(range(1, count, 2)):
            piece = core if m % 2 == 0 else other
            cp = post(held.at[piece, pl.ds(first, size)], gathered.at[d, pl.ds(first, size)], "dp", dpeers[m], lot)
            got.setdefault(m, []).append(cp)
        gathered[d, first : first + size] = held[core, first : first + size]

    igot, tgot = {}, {}
    igot_lot, tgot_lot = post.lot(dgi.at[: count - 1]), post.lot(dgt.at[: count - 1])
    ends = [post.lot(oih.at[: n - 1], True), post.lot(oth.at[:, : (n - 1) * own], True)]

    def text_half(h):
        at = slice(h * hr, (h + 1) * hr)
        up = raw[0, at]
        for r in [1] + evens:
            up = up + text_take(r, h)
        spread(lower(scale * up, tu[at], tl[at, 0:1]), dt, dgt, h * hr, tgot, tgot_lot)

    up = iup[core, chip]
    for m, cp, cq in iback:
        cp.wait_recv()
        cq.wait_recv()
        up = up + decoded(iqr[m]) * to_column(isr[m], diag)
    low = lower(scale * up, iu[...], il[:, 0:1])
    spread(low, di, dgi, 0, igot, igot_lot)
    text_half(0)
    for r in far:
        k = zpeers[r]
        ghi[r] = nt(low, ip[k]).astype(BF)
        post(ghi.at[r], oih.at[b], "branch", k, ends[0])
    oih[b] = nt(low, ip[b]).astype(BF)
    for m in range(1, count, 2):
        hin[m].wait_recv()
        yin[m].wait_recv()
    text_half(1)
    low = jnp.concatenate([dt[0], dt[1]], axis=1)
    for r in far:
        k = zpeers[r]
        ght[r] = nt(tp[k], low).astype(BF)
        post(ght.at[r], oth.at[:, pl.ds(start, own)], "branch", k, ends[1])
    oth[:, pl.ds(start, own)] = nt(tp[b], low).astype(BF)

    def product(held, got, gathered, size, out):
        y = nn(held[d].reshape(n * size, own), gathered[d])
        for m in outward + list(range(1, count, 2)):
            for cp in got[m]:
                cp.wait_recv()
            y = y + nn(held[dpeers[m]].reshape(n * size, own), gathered[dpeers[m]])
        out[...] = y.reshape(n, size, half)

    def exchange(part, wp, held, came):
        got = []
        for r in far:
            y, s = coded(wp[zpeers[r]], 0)
            held[r] = y
            zs[part, r] = s
            got.append((r, post(held.at[r], came.at[r], "branch", zpeers[r]),
                        post(zs.at[part, r], zsr.at[part, r], "branch", zpeers[r])))
        return got

    def settle(part, wp, came, got, out):
        y = wp[b]
        for r, cp, cq in got:
            cp.wait_recv()
            cq.wait_recv()
            y = y + decoded(came[r]) * zsr[part, r]
        y, s = coded(y, 0)
        out[chip, :, pl.ds(column, half)] = y
        (wsi, wst)[part][chip, :, pl.ds(column, half)] = s
        got = {}
        for m in outward + [1]:
            got[m] = pass_on(part, chip, out, dpeers[m])
        return got

    def pass_on(part, k, out, peer):
        piece = out.at[k, :, pl.ds(column, half)]
        lengths = (wsi, wst)[part].at[k, :, pl.ds(column, half)]
        return (post(piece, piece, "dp", peer), post(lengths, lengths, "dp", peer))

    def relay(part, got, out):
        for m in outward:
            for cp in got[m]:
                cp.wait_recv()
            got[m ^ 1] = pass_on(part, xor(chip, m // 2), out, dpeers[1])

    product(hxg, igot, dgi, ri, wpi)
    iz = exchange(0, wpi, zqi, zqir)
    product(hyg, tgot, dgt, rt, wpt)
    tz = exchange(1, wpt, zqt, zqtr)
    zin.wait_recv()
    y = scz[0]
    for s in range(1, n):
        y = y + scz[s]
    scd[d] = y
    din = post.lot(scd.at[: count - 1], True)
    for m in range(1, count):
        post(scd.at[d], scd.at[d], "dp", dpeers[m], din)
    ilast = settle(0, wpi, zqir, iz, wqi)
    tlast = settle(1, wpt, zqtr, tz, wqt)
    relay(0, ilast, wqi)
    relay(1, tlast, wqt)
    for lot in [din] + ends:
        lot.wait_recv()
    y = scd[0]
    for s in range(1, count):
        y = y + scd[s]
    sc_out[...] = y
    for last in (ilast, tlast):
        for m in range(1, count, 2):
            for cp in last[m]:
                cp.wait_recv()
    post.finish()
    assert post.count == sems.shape[0], (post.count, sems.shape)


def output_kernel(gih, gth, wqi, wqt, wsi, wst, sc, loss, slope, oih, oth, oi, ot):
    loss[...] = sc[0:1, 0:1]
    slope[...] = sc[1:2, 0:1]
    oih[...] = gih[...]
    oth[...] = gth[...]
    oi[...] = decoded(wqi[...]) * wsi[...]
    ot[...] = decoded(wqt[...]) * wst[...]


def per_device(image_hidden, text_hidden, image_proj, text_proj, log_inverse_sharpness, partner):
    n = lax.axis_size("branch")
    count = lax.axis_size("dp")
    chips = count // 2
    group, wide = image_hidden.shape
    thin = text_hidden.shape[1]
    own = group // n
    embed = image_proj.shape[1]
    half = embed // 2
    ri, rt = wide // chips, thin // chips
    total = group * count
    spec = pl.BlockSpec(memory_space=VMEM)
    messages = 20 + 19 * (n - 1) + 14 * (count - 1) + 5 * chips - 4
    outs = [((n, own, wide), BF), ((thin, group), BF), ((chips, ri, embed), I16), ((chips, rt, embed), I16),
            ((chips, 1, embed), F32), ((chips, 1, embed), F32), ((2, 128), F32)]
    scratch = [
        VMEM((n, own, wide), BF), VMEM((n, thin, group), BF),
        VMEM((own, embed), F32), VMEM((own, 128), F32), VMEM((own, embed), F32), VMEM((own, 128), F32),
        VMEM((count, own, embed), BF), VMEM((n, own, embed), BF), VMEM((n, own, embed), F32),
        VMEM((chips, n, own, 2 * own), F32), VMEM((group, own), F32),
        VMEM((2, chips, 1, 2 * own), F32), VMEM((count, 2, chips, 1, 2 * own), F32),
        VMEM((2, n, 1, own), F32), VMEM((n, 2, n, 1, own), F32), VMEM((chips, n, own, 2 * own), BF),
        VMEM((n, 2, own // 2, embed), I16), VMEM((n, 2, 1, own), F32),
        VMEM((n, 2, own // 2, embed), I16), VMEM((n, 2, 1, own), F32),
        VMEM((2, chips, own, embed), F32), VMEM((chips, own, embed), F32),
        VMEM((chips, own, embed), I16), VMEM((chips, 1, own), F32), VMEM((chips, own, embed), I16), VMEM((chips, 1, own), F32),
        VMEM((chips, n, ri, own), BF), VMEM((chips, n, rt, own), BF),
        VMEM((count, n, ri, own), BF), VMEM((count, n, rt, own), BF),
        VMEM((2, own, half), BF), VMEM((2, own, half), BF), VMEM((count, own, half), BF), VMEM((count, own, half), BF),
        VMEM((n, own, wide), BF), VMEM((n, thin, own), BF),
        VMEM((n, ri, half), I16), VMEM((n, rt, half), I16), VMEM((n, ri, half), I16), VMEM((n, rt, half), I16),
        VMEM((2, n, 1, half), F32), VMEM((2, n, 1, half), F32), VMEM((n, ri, half), F32), VMEM((n, rt, half), F32),
        VMEM((n, 2, 128), F32), VMEM((count, 2, 128), F32),
        VMEM((n, wide, embed), BF), VMEM((n, thin, embed), BF),
        pltpu.SemaphoreType.DMA((2,)), pltpu.SemaphoreType.DMA((messages,)),
    ]
    args = (
        image_hidden.reshape(n, own, wide), text_hidden.T,
        image_proj.reshape(n, wide, embed), text_proj.reshape(n, thin, embed),
        partner.reshape(count * n, 1, own), log_inverse_sharpness.reshape(1, 1),
    )
    gih, gth, wqi, wqt, wsi, wst, sc = pl.pallas_call(
        functools.partial(step_kernel, n, count, total),
        out_shape=[jax.ShapeDtypeStruct(s, t) for s, t in outs],
        in_specs=[spec, spec, pl.BlockSpec(memory_space=pl.ANY), pl.BlockSpec(memory_space=pl.ANY), spec, spec],
        out_specs=[spec] * len(outs),
        scratch_shapes=scratch,
        compiler_params=pltpu.CompilerParams(
            collective_id=0, has_side_effects=True, vmem_limit_bytes=60 * 1024 * 1024
        ),
    )(*args)

    loss, slope, oih, oth, oi, ot = pl.pallas_call(
        output_kernel,
        out_shape=[
            jax.ShapeDtypeStruct((1, 1), F32), jax.ShapeDtypeStruct((1, 1), F32),
            jax.ShapeDtypeStruct((n, own, wide), BF), jax.ShapeDtypeStruct((thin, group), BF),
            jax.ShapeDtypeStruct((chips, ri, embed), F32), jax.ShapeDtypeStruct((chips, rt, embed), F32),
        ],
        in_specs=[spec] * 7,
        out_specs=[spec] * 6,
    )(gih, gth, wqi, wqt, wsi, wst, sc)
    return (
        loss.reshape(1),
        slope.reshape(1),
        oih.reshape(group, wide),
        oth.T,
        oi.reshape(wide, embed),
        ot.reshape(thin, embed),
    )


def solution(mesh):
    placed = (P("dp", "branch"), P("dp", "branch"), P(), P(), P(), P())
    return jax.shard_map(
        per_device,
        mesh=mesh,
        in_specs=placed,
        out_specs=(
            P(),
            P(),
            P("dp", "branch"),
            P("dp", "branch"),
            P("branch", None),
            P("branch", None),
        ),
        check_vma=False,
    )
```
